512 devices in a mesh: tm: 128 (over z, x, core), space: 4 (over y).
Axes of the slice: x: 4, y: 4, z: 16, core: 2. Of those that a mesh axis runs over, the one named last changes fastest.
Arguments:
- state: float32 [512, 16, 64, 128], P('tm', 'space'), may hold values from -6 to 6
- source: float32 [512, 16, 64, 128], P('tm', 'space'), may hold values from -6 to 6
- absorption: float32 [16, 64, 128], P('space'), may hold values from 0.05 to 0.5
Outputs:
- relaxed: float32 [512, 16, 64, 128], P('tm', 'space')
- coarse_residual: float32 [128, 16, 64, 128], P('tm', 'space')
- residual_norm: float32 [], replicated
The draws below stay inside these ranges and needn't reach their ends.
All inputs are finite; a program needn't handle non-finite values.
Results may differ from the reference program's by a relative error of at most 0.0004.
Values sent between devices are 32-bit elements; how exact they have to be, the bound alone decides.
A program may use at most 64 MiB of HBM per device.

```python
import math
import jax
import jax.numpy as jnp

NX = 64
NY = 128
CF = 4
SWEEPS = 5
NC = 128
NT = 512
NZ = 16


def shard_levels(stream_key, dims, cuts, low, high):
    level, own = 1.0, jax.random.fold_in(stream_key, 6)
    for dim, shards_of in cuts:
        steps = jnp.exp(jax.random.uniform(jax.random.fold_in(own, dim), (shards_of,), jnp.float32, low / len(cuts), high / len(cuts)))
        level = level * jnp.repeat(steps, dims[dim] // shards_of).reshape([-1 if axis == dim else 1 for axis in range(len(dims))])
    return level


def scatter_about(key, dims, deviation, limit, split=(), kind=jnp.bfloat16):
    drawn = deviation * jax.random.normal(key, dims, jnp.float32)
    if split:
        drawn = drawn * shard_levels(key, dims, split, -0.22, 0.18)
    return jnp.clip(drawn, -limit, limit).astype(kind)


def setup_inputs(seed: int = 0) -> dict:
    arg_keys = jax.random.split(jax.random.key(seed), 4)
    return {
        "state": scatter_about(arg_keys[0], (NT, NZ, NX, NY), 1.0, 6.0, ((0, 128), (1, 4)), jnp.float32),
        "source": scatter_about(arg_keys[1], (NT, NZ, NX, NY), 1.0, 6.0, ((0, 128), (1, 4)), jnp.float32),
        "absorption": jnp.clip(jnp.exp(math.log(0.5) - 2.3025851 * jax.random.uniform(arg_keys[2], (NZ, NX, NY), jnp.float32) ** shard_levels(arg_keys[2], (NZ, NX, NY), ((0, 4),), -0.2, 0.2)), 0.05, 0.5),
    }


coupling = 4.0


def sweep_weights(count):
    spread = 6.0 * coupling / (1.0 + 6.0 * coupling)
    return [1.0 / (1.0 + spread * math.cos(math.pi * (2 * k + 1) / (2 * count))) for k in range(count)]


def apply_operator(field, diag):
    lead = [(0, 0)] * (field.ndim - 3)
    padded = jnp.pad(field, lead + [(1, 1), (1, 1), (1, 1)])
    beside = padded[..., 2:, 1:-1, 1:-1] + padded[..., :-2, 1:-1, 1:-1]
    beside = beside + padded[..., 1:-1, 2:, 1:-1] + padded[..., 1:-1, :-2, 1:-1]
    beside = beside + padded[..., 1:-1, 1:-1, 2:] + padded[..., 1:-1, 1:-1, :-2]
    return diag * field - coupling * beside


def implicit_step(rhs, diag):
    field = rhs / diag
    for weight in sweep_weights(SWEEPS):
        field = field + weight * (rhs - apply_operator(field, diag)) / diag
    return field


def reference(state, source, absorption):
    diag = 1.0 + 6.0 * coupling + absorption
    fine = state.reshape(NC, CF, NZ, NX, NY)
    rhs = source.reshape(NC, CF, NZ, NX, NY)
    points = [fine[:, j] for j in range(CF)]

    def relax_fine(points):
        for j in range(1, CF):
            points[j] = implicit_step(points[j - 1], diag) + rhs[:, j]
        return points

    def previous(last):
        return jnp.concatenate([jnp.zeros_like(last[:1]), last[:-1]], axis=0)

    points = relax_fine(points)
    points[0] = implicit_step(previous(points[-1]), diag) + rhs[:, 0]
    points = relax_fine(points)
    coarse_residual = rhs[:, 0] + implicit_step(previous(points[-1]), diag) - points[0]
    relaxed = jnp.stack(points, axis=1).reshape(NT, NZ, NX, NY)
    return relaxed, coarse_residual, jnp.sum(coarse_residual * coarse_residual)
```

```python
import math

import jax
import jax.numpy as jnp
import numpy as np
from jax import lax
from jax.experimental import pallas as pl
from jax.experimental.pallas import tpu as pltpu
from jax.sharding import PartitionSpec as P

MESH = pl.DeviceIdType.MESH
CF = 4
SWEEPS = 5
COUPLING = 4.0
NZ, NX, NY = 16, 64, 128
OWN = 4
SPACES = 4
PLANE = 8


def sweep_weights(count):
    spread = 6.0 * COUPLING / (1.0 + 6.0 * COUPLING)
    return [
        1.0 / (1.0 + spread * math.cos(math.pi * (2 * k + 1) / (2 * count))) for k in range(count)
    ]


def coefficients():
    poly = np.zeros(SWEEPS + 1)
    poly[0] = 1.0
    for w in sweep_weights(SWEEPS):
        shifted = np.concatenate([[0.0], poly[:-1]])
        poly = (1.0 - w) * poly + w * shifted
        poly[0] += w
    return [float(c) for c in poly]


COEF = coefficients()
C2 = 0.5 * (COEF[2] + COEF[3])
C4 = 0.5 * (COEF[4] + COEF[5])


def kernel(
    state, source, absorption, relaxed, residual, norm,
    a_full, u_full, s1_full, s2_full, s0_own, s3_own,
    rd, q1, q2, q3, d_buf, p_buf, w_buf, v_buf, e_full, x_buf,
    rs_left, rs_right, rv_own, rv_left, rv_right, stage, r_recv, r_stage,
    na, nb,
    local_sem, out_sem, ag_send, ag_recv, rs_send, rs_recv, v_send, v_recv,
    r_send, r_recv_sem, na_send, na_recv, nb_send, nb_recv,
):
    c = lax.axis_index("tm")
    d = lax.axis_index("space")
    tms = lax.axis_size("tm")
    levels = tms // PLANE
    after, before = lax.rem(c + 1, tms), lax.rem(c + tms - 1, tms)
    right, left = lax.rem(d + 1, SPACES), lax.rem(d + SPACES - 1, SPACES)
    opposite = lax.rem(d + 2, SPACES)
    plane, seat = c // PLANE, lax.rem(c, PLANE)
    base = d * OWN

    def at(t, s):
        return {"tm": t, "space": s}

    def seat_at(i):
        return plane * PLANE + lax.rem(seat + i, PLANE)

    def level_at(i):
        return lax.rem(plane + i, levels) * PLANE + seat

    mine = pl.ds(base, OWN)
    loads = []
    for i, (src, dst) in enumerate([
        (absorption, a_full.at[mine]),
        (state.at[0], u_full.at[mine]),
        (source.at[1], s1_full.at[mine]),
        (source.at[2], s2_full.at[mine]),
        (source.at[0], s0_own),
        (source.at[3], s3_own),
    ]):
        copy = pltpu.make_async_copy(src, dst, local_sem.at[i])
        copy.start()
        loads.append(copy)

    barrier = pltpu.get_barrier_semaphore()
    peers = [at(c, left), at(c, right)]
    peers += [at(t, s) for t in (after, before) for s in (d, left, right)]
    peers += [at(seat_at(i), d) for i in range(1, PLANE)]
    peers += [at(level_at(i), d) for i in range(1, levels)]
    for peer in peers:
        pl.semaphore_signal(barrier, inc=1, device_id=peer, device_id_type=MESH)

    rows = lax.broadcasted_iota(jnp.int32, (8, NY), 0)
    lanes = lax.broadcasted_iota(jnp.int32, (8, 8, NY), 2)

    def natural(ref, *index):
        return jnp.stack([ref[(*index, pl.ds(v, 8, stride=8), slice(None))] for v in range(8)])

    def put_natural(ref, value, *index):
        for v in range(8):
            ref[(*index, pl.ds(v, 8, stride=8), slice(None))] = value[v]

    class Gather:
        def __init__(self, full, slot):
            self.full, self.slot = full, slot

        def copy(self, layers, part, target):
            return pltpu.make_async_remote_copy(
                src_ref=self.full.at[layers], dst_ref=self.full.at[layers],
                send_sem=ag_send.at[self.slot, part], recv_sem=ag_recv.at[self.slot, part],
                device_id=target, device_id_type=MESH,
            )

        def start(self):
            self.to_right = self.copy(mine, 0, at(c, right))
            self.to_left = self.copy(mine, 1, at(c, left))
            self.to_right.start()
            self.to_left.start()

        def forward(self):
            self.copy(pl.ds(left * OWN, OWN), 0, at(c, right)).wait_recv()
            self.on_right = self.copy(pl.ds(left * OWN, 2), 2, at(c, right))
            self.on_right.start()
            self.copy(pl.ds(right * OWN, OWN), 1, at(c, left)).wait_recv()
            self.on_left = self.copy(pl.ds(right * OWN + 2, 2), 3, at(c, left))
            self.on_left.start()

        def finish(self):
            self.copy(pl.ds(opposite * OWN, 2), 2, at(c, right)).wait_recv()
            self.copy(pl.ds(opposite * OWN + 2, 2), 3, at(c, left)).wait_recv()

        def drain(self):
            for copy in (self.to_right, self.to_left, self.on_right, self.on_left):
                copy.wait_send()

    gather_a, gather_u = Gather(a_full, 0), Gather(u_full, 1)
    gather_s1, gather_s2 = Gather(s1_full, 2), Gather(s2_full, 3)
    gather_e = Gather(e_full, 4)

    def neighbours(ref, z):
        x = ref[z]
        up = jnp.where(rows == 0, 0.0, pltpu.roll(x[7], 1, 0))
        down = jnp.where(rows == 7, 0.0, pltpu.roll(x[0], 7, 0))
        total = jnp.concatenate([up[None], x[:7]]) + jnp.concatenate([x[1:], down[None]])
        total = total + jnp.where(lanes == 0, 0.0, pltpu.roll(x, 1, 2))
        total = total + jnp.where(lanes == NY - 1, 0.0, pltpu.roll(x, NY - 1, 2))
        if z > 0:
            total = total + ref[z - 1]
        if z < NZ - 1:
            total = total + ref[z + 1]
        return x, total

    def phi(emit):
        for z in range(NZ):
            p_buf[z] = q1[z] * neighbours(d_buf, z)[1]
        for z in range(NZ):
            w_buf[z] = d_buf[z] + q2[z] * neighbours(p_buf, z)[1]
        for z in range(NZ):
            p_buf[z] = q1[z] * neighbours(w_buf, z)[1]
        for z in range(NZ):
            w_buf[z] = d_buf[z] + q3[z] * neighbours(p_buf, z)[1]
        for z in range(NZ):
            x, total = neighbours(w_buf, z)
            emit(z, x + q1[z] * total)

    loads[0].wait()
    pl.semaphore_wait(barrier, len(peers))

    gather_a.start()
    for load in loads[1:]:
        load.wait()
    for z in range(NZ):
        d_buf[z] = jnp.zeros((8, 8, NY), jnp.float32)
    gather_a.forward()
    gather_u.start()
    gather_a.finish()
    for z in range(NZ):
        inverse = 1.0 / (1.0 + 6.0 * COUPLING + natural(a_full, z))
        rd[z] = inverse
        q1[z] = COUPLING * inverse
        q2[z] = (COUPLING * C4 / C2) * inverse
        q3[z] = (COUPLING * C2) * inverse

    for k in range(OWN):
        d_buf[base + k] = rd[base + k] * natural(u_full, base + k)

    def scaled(z, x):
        d_buf[z] = rd[z] * x

    for own in (
        lambda k: natural(s1_full, base + k),
        lambda k: natural(s2_full, base + k),
        lambda k: natural(s3_own, k),
    ):
        phi(scaled)
        for k in range(OWN):
            d_buf[base + k] = d_buf[base + k] + rd[base + k] * own(k)

    def respond(z, x):
        v_buf[z] = x

    phi(respond)
    gather_u.forward()

    def remote(src, dst, send, recv, target):
        return pltpu.make_async_remote_copy(
            src_ref=src, dst_ref=dst, send_sem=send, recv_sem=recv,
            device_id=target, device_id_type=MESH,
        )

    part_right = remote(v_buf.at[pl.ds(opposite * OWN, 2)], rs_left,
                        rs_send.at[0], rs_recv.at[0], at(c, right))
    part_left = remote(v_buf.at[pl.ds(opposite * OWN + 2, 2)], rs_right,
                       rs_send.at[1], rs_recv.at[1], at(c, left))
    part_right.start()
    part_left.start()
    v_own = remote(v_buf.at[mine], rv_own, v_send.at[0], v_recv.at[0], at(after, d))
    v_own.start()
    v_right_late = remote(v_buf.at[pl.ds(right * OWN + 2, 2)], rv_left.at[pl.ds(2, 2)],
                          v_send.at[1], v_recv.at[1], at(after, right))
    v_left_late = remote(v_buf.at[pl.ds(left * OWN, 2)], rv_right.at[pl.ds(0, 2)],
                         v_send.at[2], v_recv.at[2], at(after, left))
    v_right_late.start()
    v_left_late.start()
    part_right.wait_recv()
    for k in range(2):
        v_buf[right * OWN + k] = v_buf[right * OWN + k] + rs_left[k]
    v_right = remote(v_buf.at[pl.ds(right * OWN, 2)], rv_left.at[pl.ds(0, 2)],
                     v_send.at[3], v_recv.at[3], at(after, right))
    v_right.start()
    part_left.wait_recv()
    for k in range(2):
        v_buf[left * OWN + 2 + k] = v_buf[left * OWN + 2 + k] + rs_right[k]
    v_left = remote(v_buf.at[pl.ds(left * OWN + 2, 2)], rv_right.at[pl.ds(2, 2)],
                    v_send.at[4], v_recv.at[4], at(after, left))
    v_left.start()

    gather_u.finish()
    for z in range(NZ):
        d_buf[z] = rd[z] * natural(u_full, z)

    def first(z, x):
        x_buf[4, z] = x

    phi(first)

    for copy in (v_own, v_right_late, v_left_late, v_right, v_left):
        copy.wait_recv()
    has_before = jnp.where(c > 0, 1.0, 0.0).astype(jnp.float32)
    for k in range(OWN):
        q = has_before * (rv_own[k] + rv_left[k] + rv_right[k])
        point = q + natural(s0_own, k)
        put_natural(stage, point, 0, k)
        e_full[base + k] = point - natural(u_full, base + k)
    gather_e.start()
    outs = [pltpu.make_async_copy(stage.at[0], relaxed.at[0], out_sem.at[0])]
    outs[0].start()
    gather_e.forward()
    gather_s1.start()
    gather_e.finish()

    for z in range(NZ):
        d_buf[z] = rd[z] * e_full[z]

    def chain(j):
        def emit(z, x):
            x_buf[j, z] = x
            d_buf[z] = rd[z] * x
        return emit

    for j in range(CF - 1):
        phi(chain(j))

    squares = []

    def last(z, x):
        x_buf[3, z] = x
        squares.append(x * x)

    phi(last)
    total = squares[0]
    for square in squares[1:]:
        total = total + square
    has_after = jnp.where(c < tms - 1, 1.0, 0.0).astype(jnp.float32)
    na[0] = has_after * jnp.sum(jnp.sum(total, axis=0), axis=0, keepdims=True)
    na_copies = []
    for i in range(1, PLANE):
        copy = remote(na.at[0], na.at[i], na_send.at[i - 1], na_recv.at[i - 1], at(seat_at(i), d))
        copy.start()
        na_copies.append(copy)
    r_copy = remote(x_buf.at[3, mine], r_recv, r_send.at[0], r_recv_sem.at[0], at(after, d))
    r_copy.start()
    gather_s1.forward()
    gather_s2.start()
    for copy in na_copies:
        copy.wait_recv()
    row = na[0]
    for i in range(1, PLANE):
        row = row + na[i]
    nb[0] = row
    nb_copies = []
    for i in range(1, levels):
        copy = remote(nb.at[0], nb.at[i], nb_send.at[i - 1], nb_recv.at[i - 1], at(level_at(i), d))
        copy.start()
        nb_copies.append(copy)

    gather_s1.finish()
    for z in range(NZ):
        d_buf[z] = rd[z] * (x_buf[4, z] + natural(s1_full, z))
    for k in range(OWN):
        value = x_buf[4, base + k] + natural(s1_full, base + k) + x_buf[0, base + k]
        put_natural(stage, value, 1, k)
    outs.append(pltpu.make_async_copy(stage.at[1], relaxed.at[1], out_sem.at[1]))
    outs[1].start()
    gather_s2.forward()
    phi(first)
    gather_s2.finish()
    for z in range(NZ):
        d_buf[z] = rd[z] * (x_buf[4, z] + natural(s2_full, z))
    for k in range(OWN):
        value = x_buf[4, base + k] + natural(s2_full, base + k) + x_buf[1, base + k]
        put_natural(stage, value, 2, k)
    outs.append(pltpu.make_async_copy(stage.at[2], relaxed.at[2], out_sem.at[2]))
    outs[2].start()
    phi(first)
    for k in range(OWN):
        value = x_buf[4, base + k] + natural(s3_own, k) + x_buf[2, base + k]
        put_natural(stage, value, 3, k)
    outs.append(pltpu.make_async_copy(stage.at[3], relaxed.at[3], out_sem.at[3]))
    outs[3].start()

    r_copy.wait_recv()
    for k in range(OWN):
        put_natural(r_stage, has_before * r_recv[k], k)
    outs.append(pltpu.make_async_copy(r_stage, residual.at[0], out_sem.at[4]))
    outs[4].start()

    for copy in nb_copies:
        copy.wait_recv()
    row = nb[0]
    for i in range(1, levels):
        row = row + nb[i]
    norm[...] = jnp.broadcast_to(jnp.sum(row, axis=1, keepdims=True), (1, NY))

    for gather in (gather_a, gather_u, gather_s1, gather_s2, gather_e):
        gather.drain()
    for copy in (part_right, part_left, v_own, v_right_late, v_left_late, v_right, v_left, r_copy):
        copy.wait_send()
    for copy in na_copies + nb_copies:
        copy.wait_send()
    for copy in outs:
        copy.wait()


def local(state, source, absorption):
    levels = lax.axis_size("tm") // PLANE
    f32 = jnp.float32
    packed = (NZ, 8, 8, NY)
    any_spec = pl.BlockSpec(memory_space=pl.ANY)
    vm = lambda *shape: pltpu.VMEM(shape, f32)
    dma = lambda *shape: pltpu.SemaphoreType.DMA(shape)
    relaxed, residual, norm = pl.pallas_call(
        kernel,
        out_shape=(
            jax.ShapeDtypeStruct((CF, OWN, NX, NY), f32),
            jax.ShapeDtypeStruct((1, OWN, NX, NY), f32),
            jax.ShapeDtypeStruct((1, NY), f32),
        ),
        in_specs=[any_spec] * 3,
        out_specs=(any_spec, any_spec, pl.BlockSpec(memory_space=pltpu.VMEM)),
        scratch_shapes=[
            vm(NZ, NX, NY), vm(NZ, NX, NY), vm(NZ, NX, NY), vm(NZ, NX, NY),
            vm(OWN, NX, NY), vm(OWN, NX, NY),
            vm(*packed), vm(*packed), vm(*packed), vm(*packed),
            vm(*packed), vm(*packed), vm(*packed), vm(*packed), vm(*packed),
            vm(5, *packed),
            vm(2, 8, 8, NY), vm(2, 8, 8, NY),
            vm(OWN, 8, 8, NY), vm(OWN, 8, 8, NY), vm(OWN, 8, 8, NY),
            vm(CF, OWN, NX, NY), vm(OWN, 8, 8, NY), vm(OWN, NX, NY),
            vm(PLANE, 1, NY), vm(levels, 1, NY),
            dma(6), dma(5), dma(5, 4), dma(5, 4), dma(2), dma(2), dma(5), dma(5),
            dma(1), dma(1), dma(PLANE - 1), dma(PLANE - 1), dma(levels - 1), dma(levels - 1),
        ],
        compiler_params=pltpu.CompilerParams(
            collective_id=0, has_side_effects=True, vmem_limit_bytes=32 * 1024 * 1024
        ),
    )(state, source, absorption)
    return relaxed, residual, norm[0, 0]


def solution(mesh):
    return jax.shard_map(
        local,
        mesh=mesh,
        in_specs=(P("tm", "space", None, None), P("tm", "space", None, None), P("space", None, None)),
        out_specs=(P("tm", "space", None, None), P("tm", "space", None, None), P()),
        check_vma=False,
    )
```

```python
import math

import jax
import jax.numpy as jnp
import numpy as np
from jax import lax
from jax.experimental import pallas as pl
from jax.experimental.pallas import tpu as pltpu
from jax.sharding import PartitionSpec as P

MESH = pl.DeviceIdType.MESH
CF = 4
SWEEPS = 5
COUPLING = 4.0
NZ, NX, NY = 16, 64, 128
OWN = 4
SPACES = 4
PLANE = 8
READY = 3
VMEM_BYTES = 67043328


def sweep_weights(count):
    spread = 6.0 * COUPLING / (1.0 + 6.0 * COUPLING)
    return [
        1.0 / (1.0 + spread * math.cos(math.pi * (2 * k + 1) / (2 * count))) for k in range(count)
    ]


def coefficients():
    poly = np.zeros(SWEEPS + 1)
    poly[0] = 1.0
    for w in sweep_weights(SWEEPS):
        shifted = np.concatenate([[0.0], poly[:-1]])
        poly = (1.0 - w) * poly + w * shifted
        poly[0] += w
    return [float(c) for c in poly]


COEF = coefficients()
C2 = 0.5 * (COEF[2] + COEF[3])
C4 = 0.5 * (COEF[4] + COEF[5])


def kernel(
    state, source, absorption, relaxed, residual, norm,
    a_full, u_full, s1_full, s2_full, s0_own, s3_own,
    rd, q1, q2, q3, d_buf, p_buf, w_buf, v_buf, e_full, x_buf,
    rs_left, rs_right, rv_own, rv_left, rv_right, stage, r_recv, r_stage,
    na, nb,
    local_sem, out_sem, ag_send, ag_recv, rs_send, rs_recv, v_send, v_recv,
    r_send, r_recv_sem, na_send, na_recv, nb_send, nb_recv, ready_sem,
):
    c = lax.axis_index("tm")
    d = lax.axis_index("space")
    tms = lax.axis_size("tm")
    levels = tms // PLANE
    after, before = lax.rem(c + 1, tms), lax.rem(c + tms - 1, tms)
    right, left = lax.rem(d + 1, SPACES), lax.rem(d + SPACES - 1, SPACES)
    opposite = lax.rem(d + 2, SPACES)
    plane, seat = c // PLANE, lax.rem(c, PLANE)
    base = d * OWN

    def at(t, s):
        return {"tm": t, "space": s}

    def seat_at(i):
        return plane * PLANE + lax.rem(seat + i, PLANE)

    def level_at(i):
        return lax.rem(plane + i, levels) * PLANE + seat

    mine = pl.ds(base, OWN)
    loads = []
    for i, (src, dst) in enumerate([
        (absorption, a_full.at[mine]),
        (state.at[0], u_full.at[mine]),
        (source.at[1], s1_full.at[mine]),
        (source.at[2], s2_full.at[mine]),
        (source.at[0], s0_own),
        (source.at[3], s3_own),
    ]):
        copy = pltpu.make_async_copy(src, dst, local_sem.at[i])
        copy.start()
        loads.append(copy)

    barrier = pltpu.get_barrier_semaphore()
    peers = [at(c, left), at(c, right)]
    peers += [at(t, s) for t in (after, before) for s in (d, left, right)]
    peers += [at(seat_at(i), d) for i in range(1, PLANE)]
    peers += [at(level_at(i), d) for i in (1, levels - 1)]
    for peer in peers:
        pl.semaphore_signal(barrier, inc=1, device_id=peer, device_id_type=MESH)

    rows = lax.broadcasted_iota(jnp.int32, (8, NY), 0)
    lanes = lax.broadcasted_iota(jnp.int32, (8, 8, NY), 2)

    def natural(ref, *index):
        return jnp.stack([ref[(*index, pl.ds(v, 8, stride=8), slice(None))] for v in range(8)])

    def put_natural(ref, value, *index):
        for v in range(8):
            ref[(*index, pl.ds(v, 8, stride=8), slice(None))] = value[v]

    def ready_signal(stage):
        reach = 2 ** stage
        for i in (reach, levels - reach):
            pl.semaphore_signal(ready_sem.at[stage], inc=1, device_id=at(level_at(i), d), device_id_type=MESH)

    def ready_wait(stage):
        pl.semaphore_wait(ready_sem.at[stage], 2)

    class Gather:
        def __init__(self, full, slot):
            self.full, self.slot = full, slot

        def copy(self, layers, part, target):
            return pltpu.make_async_remote_copy(
                src_ref=self.full.at[layers], dst_ref=self.full.at[layers],
                send_sem=ag_send.at[self.slot, part], recv_sem=ag_recv.at[self.slot, part],
                device_id=target, device_id_type=MESH,
            )

        def start(self):
            self.to_right = self.copy(mine, 0, at(c, right))
            self.to_left = self.copy(mine, 1, at(c, left))
            self.to_right.start()
            self.to_left.start()

        def forward(self):
            self.copy(pl.ds(left * OWN, OWN), 0, at(c, right)).wait_recv()
            self.on_right = self.copy(pl.ds(left * OWN, 2), 2, at(c, right))
            self.on_right.start()
            self.copy(pl.ds(right * OWN, OWN), 1, at(c, left)).wait_recv()
            self.on_left = self.copy(pl.ds(right * OWN + 2, 2), 3, at(c, left))
            self.on_left.start()

        def finish(self):
            self.copy(pl.ds(opposite * OWN, 2), 2, at(c, right)).wait_recv()
            self.copy(pl.ds(opposite * OWN + 2, 2), 3, at(c, left)).wait_recv()

        def drain(self):
            for copy in (self.to_right, self.to_left, self.on_right, self.on_left):
                copy.wait_send()

    gather_a, gather_u = Gather(a_full, 0), Gather(u_full, 1)
    gather_s1, gather_s2 = Gather(s1_full, 2), Gather(s2_full, 3)
    gather_e = Gather(e_full, 4)

    def neighbours(ref, z):
        x = ref[z]
        up = jnp.where(rows == 0, 0.0, pltpu.roll(x[7], 1, 0))
        down = jnp.where(rows == 7, 0.0, pltpu.roll(x[0], 7, 0))
        total = jnp.concatenate([up[None], x[:7]]) + jnp.concatenate([x[1:], down[None]])
        total = total + jnp.where(lanes == 0, 0.0, pltpu.roll(x, 1, 2))
        total = total + jnp.where(lanes == NY - 1, 0.0, pltpu.roll(x, NY - 1, 2))
        if z > 0:
            total = total + ref[z - 1]
        if z < NZ - 1:
            total = total + ref[z + 1]
        return x, total

    def phi(emit):
        for z in range(NZ):
            p_buf[z] = q1[z] * neighbours(d_buf, z)[1]
        for z in range(NZ):
            w_buf[z] = d_buf[z] + q2[z] * neighbours(p_buf, z)[1]
        for z in range(NZ):
            p_buf[z] = q1[z] * neighbours(w_buf, z)[1]
        for z in range(NZ):
            w_buf[z] = d_buf[z] + q3[z] * neighbours(p_buf, z)[1]
        for z in range(NZ):
            x, total = neighbours(w_buf, z)
            emit(z, x + q1[z] * total)

    loads[0].wait()
    pl.semaphore_wait(barrier, len(peers))

    gather_a.start()
    ready_signal(0)
    for load in loads[1:]:
        load.wait()
    for z in range(NZ):
        d_buf[z] = jnp.zeros((8, 8, NY), jnp.float32)
    gather_a.forward()
    gather_u.start()
    gather_a.finish()
    ready_wait(0)
    ready_signal(1)
    for z in range(NZ):
        inverse = 1.0 / (1.0 + 6.0 * COUPLING + natural(a_full, z))
        rd[z] = inverse
        q1[z] = COUPLING * inverse
        q2[z] = (COUPLING * C4 / C2) * inverse
        q3[z] = (COUPLING * C2) * inverse

    for k in range(OWN):
        d_buf[base + k] = rd[base + k] * natural(u_full, base + k)

    def scaled(z, x):
        d_buf[z] = rd[z] * x

    for own in (
        lambda k: natural(s1_full, base + k),
        lambda k: natural(s2_full, base + k),
        lambda k: natural(s3_own, k),
    ):
        phi(scaled)
        for k in range(OWN):
            d_buf[base + k] = d_buf[base + k] + rd[base + k] * own(k)

    def respond(z, x):
        v_buf[z] = x

    phi(respond)
    gather_u.forward()

    ready_wait(1)
    ready_signal(2)

    def remote(src, dst, send, recv, target):
        return pltpu.make_async_remote_copy(
            src_ref=src, dst_ref=dst, send_sem=send, recv_sem=recv,
            device_id=target, device_id_type=MESH,
        )

    part_right = remote(v_buf.at[pl.ds(opposite * OWN, 2)], rs_left,
                        rs_send.at[0], rs_recv.at[0], at(c, right))
    part_left = remote(v_buf.at[pl.ds(opposite * OWN + 2, 2)], rs_right,
                       rs_send.at[1], rs_recv.at[1], at(c, left))
    part_right.start()
    part_left.start()
    v_own = remote(v_buf.at[mine], rv_own, v_send.at[0], v_recv.at[0], at(after, d))
    v_own.start()
    v_right_late = remote(v_buf.at[pl.ds(right * OWN + 2, 2)], rv_left.at[pl.ds(2, 2)],
                          v_send.at[1], v_recv.at[1], at(after, right))
    v_left_late = remote(v_buf.at[pl.ds(left * OWN, 2)], rv_right.at[pl.ds(0, 2)],
                         v_send.at[2], v_recv.at[2], at(after, left))
    v_right_late.start()
    v_left_late.start()
    part_right.wait_recv()
    for k in range(2):
        v_buf[right * OWN + k] = v_buf[right * OWN + k] + rs_left[k]
    v_right = remote(v_buf.at[pl.ds(right * OWN, 2)], rv_left.at[pl.ds(0, 2)],
                     v_send.at[3], v_recv.at[3], at(after, right))
    v_right.start()
    part_left.wait_recv()
    for k in range(2):
        v_buf[left * OWN + 2 + k] = v_buf[left * OWN + 2 + k] + rs_right[k]
    v_left = remote(v_buf.at[pl.ds(left * OWN + 2, 2)], rv_right.at[pl.ds(2, 2)],
                    v_send.at[4], v_recv.at[4], at(after, left))
    v_left.start()

    gather_u.finish()
    for z in range(NZ):
        d_buf[z] = rd[z] * natural(u_full, z)

    def first(z, x):
        x_buf[4, z] = x

    phi(first)

    for copy in (v_own, v_right_late, v_left_late, v_right, v_left):
        copy.wait_recv()
    has_before = jnp.where(c > 0, 1.0, 0.0).astype(jnp.float32)
    for k in range(OWN):
        q = has_before * (rv_own[k] + rv_left[k] + rv_right[k])
        point = q + natural(s0_own, k)
        put_natural(stage, point, 0, k)
        e_full[base + k] = point - natural(u_full, base + k)
    gather_e.start()
    outs = [pltpu.make_async_copy(stage.at[0], relaxed.at[0], out_sem.at[0])]
    outs[0].start()
    gather_e.forward()
    gather_s1.start()
    gather_e.finish()

    for z in range(NZ):
        d_buf[z] = rd[z] * e_full[z]

    def chain(j):
        def emit(z, x):
            x_buf[j, z] = x
            d_buf[z] = rd[z] * x
        return emit

    for j in range(CF - 1):
        phi(chain(j))
        if j == 1:
            gather_s1.forward()
            gather_s2.start()
    gather_s2.forward()
    ready_wait(2)

    squares = []

    def last(z, x):
        x_buf[3, z] = x
        squares.append(x * x)

    phi(last)
    total = squares[0]
    for square in squares[1:]:
        total = total + square
    has_after = jnp.where(c < tms - 1, 1.0, 0.0).astype(jnp.float32)
    na[0] = has_after * jnp.sum(jnp.sum(total, axis=0), axis=0, keepdims=True)
    na_copies = []
    for i in range(1, PLANE):
        copy = remote(na.at[0], na.at[i], na_send.at[i - 1], na_recv.at[i - 1], at(seat_at(i), d))
        copy.start()
        na_copies.append(copy)
    r_copy = remote(x_buf.at[3, mine], r_recv, r_send.at[0], r_recv_sem.at[0], at(after, d))
    r_copy.start()
    gather_s1.finish()
    for z in range(NZ):
        d_buf[z] = rd[z] * (x_buf[4, z] + natural(s1_full, z))
    for copy in na_copies:
        copy.wait_recv()
    row = na[0]
    for i in range(1, PLANE):
        row = row + na[i]
    nb[0] = row
    nb_copies = []
    for i in range(1, levels):
        copy = remote(nb.at[0], nb.at[i], nb_send.at[i - 1], nb_recv.at[i - 1], at(level_at(i), d))
        copy.start()
        nb_copies.append(copy)

    for k in range(OWN):
        value = x_buf[4, base + k] + natural(s1_full, base + k) + x_buf[0, base + k]
        put_natural(stage, value, 1, k)
    outs.append(pltpu.make_async_copy(stage.at[1], relaxed.at[1], out_sem.at[1]))
    outs[1].start()
    phi(first)
    gather_s2.finish()
    for z in range(NZ):
        d_buf[z] = rd[z] * (x_buf[4, z] + natural(s2_full, z))
    for k in range(OWN):
        value = x_buf[4, base + k] + natural(s2_full, base + k) + x_buf[1, base + k]
        put_natural(stage, value, 2, k)
    outs.append(pltpu.make_async_copy(stage.at[2], relaxed.at[2], out_sem.at[2]))
    outs[2].start()
    phi(first)
    for k in range(OWN):
        value = x_buf[4, base + k] + natural(s3_own, k) + x_buf[2, base + k]
        put_natural(stage, value, 3, k)
    outs.append(pltpu.make_async_copy(stage.at[3], relaxed.at[3], out_sem.at[3]))
    outs[3].start()

    r_copy.wait_recv()
    for k in range(OWN):
        put_natural(r_stage, has_before * r_recv[k], k)
    outs.append(pltpu.make_async_copy(r_stage, residual.at[0], out_sem.at[4]))
    outs[4].start()

    for copy in nb_copies:
        copy.wait_recv()
    row = nb[0]
    for i in range(1, levels):
        row = row + nb[i]
    norm[...] = jnp.broadcast_to(jnp.sum(row, axis=1, keepdims=True), (1, NY))

    for gather in (gather_a, gather_u, gather_s1, gather_s2, gather_e):
        gather.drain()
    for copy in (part_right, part_left, v_own, v_right_late, v_left_late, v_right, v_left, r_copy):
        copy.wait_send()
    for copy in na_copies + nb_copies:
        copy.wait_send()
    for copy in outs:
        copy.wait()


def local(state, source, absorption):
    levels = lax.axis_size("tm") // PLANE
    f32 = jnp.float32
    packed = (NZ, 8, 8, NY)
    any_spec = pl.BlockSpec(memory_space=pl.ANY)
    vm = lambda *shape: pltpu.VMEM(shape, f32)
    dma = lambda *shape: pltpu.SemaphoreType.DMA(shape)
    relaxed, residual, norm = pl.pallas_call(
        kernel,
        out_shape=(
            jax.ShapeDtypeStruct((CF, OWN, NX, NY), f32),
            jax.ShapeDtypeStruct((1, OWN, NX, NY), f32),
            jax.ShapeDtypeStruct((1, NY), f32),
        ),
        in_specs=[any_spec] * 3,
        out_specs=(any_spec, any_spec, pl.BlockSpec(memory_space=pltpu.VMEM)),
        scratch_shapes=[
            vm(NZ, NX, NY), vm(NZ, NX, NY), vm(NZ, NX, NY), vm(NZ, NX, NY),
            vm(OWN, NX, NY), vm(OWN, NX, NY),
            vm(*packed), vm(*packed), vm(*packed), vm(*packed),
            vm(*packed), vm(*packed), vm(*packed), vm(*packed), vm(*packed),
            vm(5, *packed),
            vm(2, 8, 8, NY), vm(2, 8, 8, NY),
            vm(OWN, 8, 8, NY), vm(OWN, 8, 8, NY), vm(OWN, 8, 8, NY),
            vm(CF, OWN, NX, NY), vm(OWN, 8, 8, NY), vm(OWN, NX, NY),
            vm(PLANE, 1, NY), vm(levels, 1, NY),
            dma(6), dma(5), dma(5, 4), dma(5, 4), dma(2), dma(2), dma(5), dma(5),
            dma(1), dma(1), dma(PLANE - 1), dma(PLANE - 1), dma(levels - 1), dma(levels - 1),
            pltpu.SemaphoreType.REGULAR((READY,)),
        ],
        compiler_params=pltpu.CompilerParams(
            collective_id=0, has_side_effects=True, vmem_limit_bytes=VMEM_BYTES
        ),
    )(state, source, absorption)
    return relaxed, residual, norm[0, 0]


def solution(mesh):
    return jax.shard_map(
        local,
        mesh=mesh,
        in_specs=(P("tm", "space", None, None), P("tm", "space", None, None), P("space", None, None)),
        out_specs=(P("tm", "space", None, None), P("tm", "space", None, None), P()),
        check_vma=False,
    )
```

```python
import math

import jax
import jax.numpy as jnp
import numpy as np
from jax import lax
from jax.experimental import pallas as pl
from jax.experimental.pallas import tpu as pltpu
from jax.sharding import PartitionSpec as P

MESH = pl.DeviceIdType.MESH
CF = 4
SWEEPS = 5
COUPLING = 4.0
NZ, NX, NY = 16, 64, 128
OWN = 4
SPACES = 4
PLANE = 8
REACHES = (1, 2, 4, 1)
COLUMNS = 4
ALL = frozenset(range(16))
VMEM_BYTES = 54272 * 1024


def sweep_weights(count):
    spread = 6.0 * COUPLING / (1.0 + 6.0 * COUPLING)
    return [
        1.0 / (1.0 + spread * math.cos(math.pi * (2 * k + 1) / (2 * count))) for k in range(count)
    ]


def coefficients():
    poly = np.zeros(SWEEPS + 1)
    poly[0] = 1.0
    for w in sweep_weights(SWEEPS):
        shifted = np.concatenate([[0.0], poly[:-1]])
        poly = (1.0 - w) * poly + w * shifted
        poly[0] += w
    return [float(c) for c in poly]


COEF = coefficients()
C2 = 0.5 * (COEF[2] + COEF[3])
C4 = 0.5 * (COEF[4] + COEF[5])


def grow(layers):
    return frozenset((z + step) % NZ for z in layers for step in (-1, 0, 1))


def kernel(
    state, source, absorption, relaxed, residual, norm,
    a_full, u_full, s1_full, s2_full, s0_own, s3_own,
    rd, q1, q2, q3, d_buf, l1, l2, l3, l4, v_buf, e_full, x_buf,
    rs_left, rs_right, rv_own, rv_left, rv_right, stage, r_recv, r_stage,
    na, nb,
    local_sem, out_sem, a_send, a_recv, ag_send, ag_recv, rs_send, rs_recv, v_send, v_recv,
    r_send, r_recv_sem, na_send, na_recv, nb_send, nb_recv, ready_sem,
):
    c = lax.axis_index("tm")
    d = lax.axis_index("space")
    tms = lax.axis_size("tm")
    levels = tms // PLANE
    after, before = lax.rem(c + 1, tms), lax.rem(c + tms - 1, tms)
    right, left = lax.rem(d + 1, SPACES), lax.rem(d + SPACES - 1, SPACES)
    plane, seat = c // PLANE, lax.rem(c, PLANE)
    core = lax.rem(c, 2)
    partner = c + 1 - 2 * core

    def at(t, s):
        return {"tm": t, "space": s}

    def seat_at(i):
        return plane * PLANE + lax.rem(seat + i, PLANE)

    def level_at(i):
        return lax.rem(plane + i, levels) * PLANE + seat

    def remote(src, dst, send, recv, target):
        return pltpu.make_async_remote_copy(
            src_ref=src, dst_ref=dst, send_sem=send, recv_sem=recv,
            device_id=target, device_id_type=MESH,
        )

    loads = []
    for i, (src, dst) in enumerate([
        (absorption, a_full.at[pl.ds(0, OWN)]),
        (state.at[0], u_full.at[pl.ds(0, OWN)]),
        (source.at[1], s1_full.at[pl.ds(0, OWN)]),
        (source.at[2], s2_full.at[pl.ds(0, OWN)]),
        (source.at[0], s0_own),
        (source.at[3], s3_own),
    ]):
        copy = pltpu.make_async_copy(src, dst, local_sem.at[i])
        copy.start()
        loads.append(copy)

    barrier = pltpu.get_barrier_semaphore()
    peers = [at(c, left), at(c, right)]
    peers += [at(t, s) for t in (after, before) for s in (d, left, right)]
    peers += [at(seat_at(i), d) for i in range(1, PLANE)]
    peers += [at(level_at(i), d) for i in (1, levels - 1)]
    for peer in peers:
        pl.semaphore_signal(barrier, inc=1, device_id=peer, device_id_type=MESH)

    rows = lax.broadcasted_iota(jnp.int32, (8, NY), 0)
    lanes = lax.broadcasted_iota(jnp.int32, (8, 8, NY), 2)
    joined = [jnp.where(d == SPACES - 1 - b, 0.0, 1.0).astype(jnp.float32) for b in range(SPACES)]

    def natural(ref, *index):
        return jnp.stack([ref[(*index, pl.ds(v, 8, stride=8), slice(None))] for v in range(8)])

    def put_natural(ref, value, *index):
        for v in range(8):
            ref[(*index, pl.ds(v, 8, stride=8), slice(None))] = value[v]

    def ready_signal(number):
        reach = REACHES[number]
        for i in (reach, levels - reach):
            pl.semaphore_signal(ready_sem.at[number], inc=1, device_id=at(level_at(i), d), device_id_type=MESH)

    def ready_wait(number):
        pl.semaphore_wait(ready_sem.at[number], 2)

    class Gather:
        def __init__(self, full, slot):
            self.full, self.slot = full, slot

        def copy(self, src, dst, count, part, target):
            return remote(self.full.at[pl.ds(src, count)], self.full.at[pl.ds(dst, count)],
                          ag_send.at[self.slot, part], ag_recv.at[self.slot, part], at(c, target))

        def start(self):
            self.copies = [self.copy(0, 12, 4, 0, right), self.copy(0, 4, 4, 1, left)]
            self.copies[0].start()
            self.copies[1].start()

        def forward(self):
            self.copies += [self.copy(12, 8, 2, 2, right), self.copy(6, 10, 2, 3, left)]
            self.copies[0].wait_recv()
            self.copies[2].start()
            self.copies[1].wait_recv()
            self.copies[3].start()

        def finish(self):
            self.copies[2].wait_recv()
            self.copies[3].wait_recv()

        def drain(self):
            for copy in self.copies:
                copy.wait_send()

    gather_u, gather_s1, gather_s2 = Gather(u_full, 0), Gather(s1_full, 1), Gather(s2_full, 2)
    gather_e = Gather(e_full, 3)

    half = 2 * core

    def a_copy(src, dst, count, part, target):
        return remote(a_full.at[pl.ds(src, count)], a_full.at[pl.ds(dst, count)],
                      a_send.at[part], a_recv.at[part], target)

    a_right = a_copy(half, 12 + half, 2, 0, at(c, right))
    a_left = a_copy(half, 4 + half, 2, 1, at(c, left))
    a_on_right = a_copy(12 + half, 8 + half, 1, 2, at(c, right))
    a_on_left = a_copy(4 + half + 1, 8 + half + 1, 1, 3, at(c, left))
    a_give_left = a_copy(12 + half, 12 + half, 2, 4, at(partner, d))
    a_give_right = a_copy(4 + half, 4 + half, 2, 5, at(partner, d))
    a_give_first = a_copy(8 + half, 8 + half, 1, 6, at(partner, d))
    a_give_second = a_copy(8 + half + 1, 8 + half + 1, 1, 7, at(partner, d))

    def neighbours(ref, z, have):
        terms = []
        if z in have:
            x = ref[z]
            up = jnp.where(rows == 0, 0.0, pltpu.roll(x[7], 1, 0))
            down = jnp.where(rows == 7, 0.0, pltpu.roll(x[0], 7, 0))
            terms.append(jnp.concatenate([up[None], x[:7]]) + jnp.concatenate([x[1:], down[None]]))
            terms.append(jnp.where(lanes == 0, 0.0, pltpu.roll(x, 1, 2)))
            terms.append(jnp.where(lanes == NY - 1, 0.0, pltpu.roll(x, NY - 1, 2)))
        above, below = (z + 1) % NZ, (z - 1) % NZ
        if above in have:
            terms.append(ref[above] if above % OWN else joined[z // OWN] * ref[above])
        if below in have:
            terms.append(ref[below] if z % OWN else joined[below // OWN] * ref[below])
        total = terms[0]
        for term in terms[1:]:
            total = total + term
        return total

    steps = [(d_buf, l1, q1), (l1, l2, q2), (l2, l3, q1), (l3, l4, q3)]

    def level(number, layers, have, have_d):
        src, dst, factor = steps[number - 1]
        for z in sorted(layers):
            value = factor[z] * neighbours(src, z, have)
            if number % 2 == 0 and z in have_d:
                value = d_buf[z] + value
            dst[z] = value

    def last_step(layers, have, emit):
        for z in sorted(layers):
            value = q1[z] * neighbours(l4, z, have)
            emit(z, l4[z] + value if z in have else value)

    def phi(emit, want=ALL):
        need = [frozenset(want)]
        for _ in range(SWEEPS - 1):
            need.insert(0, grow(need[0]))
        for number in range(1, SWEEPS):
            level(number, need[number - 1], ALL, ALL)
        last_step(want, ALL, emit)

    def invert(layers):
        for z in layers:
            inverse = 1.0 / (1.0 + 6.0 * COUPLING + natural(a_full, z))
            rd[z] = inverse
            q1[z] = COUPLING * inverse
            q2[z] = (COUPLING * C4 / C2) * inverse
            q3[z] = (COUPLING * C2) * inverse

    loads[0].wait()
    pl.semaphore_wait(barrier, len(peers))

    a_right.start()
    a_left.start()
    ready_signal(0)
    for load in loads[1:]:
        load.wait()
    invert(range(4))
    for k in range(OWN):
        d_buf[k] = rd[k] * natural(u_full, k)
    a_right.wait_recv()
    a_on_right.start()
    a_give_left.start()
    a_left.wait_recv()
    a_on_left.start()
    a_give_right.start()
    gather_u.start()
    a_give_left.wait_recv()
    a_give_right.wait_recv()
    invert((4, 5, 6, 7, 12, 13, 14, 15))

    reach = [frozenset(range(OWN))]
    for _ in range(SWEEPS):
        reach.append(grow(reach[-1]))
    for number in range(1, SWEEPS):
        level(number, reach[number], reach[number - 1], reach[0])
    a_on_right.wait_recv()
    a_give_first.start()
    a_on_left.wait_recv()
    a_give_second.start()
    a_give_first.wait_recv()
    a_give_second.wait_recv()
    invert((8, 9, 10, 11))
    for z in ALL - reach[SWEEPS]:
        d_buf[z] = jnp.zeros((8, 8, NY), jnp.float32)

    def scaled(z, x):
        d_buf[z] = rd[z] * x

    last_step(reach[SWEEPS], reach[SWEEPS - 1], scaled)
    for k in range(OWN):
        d_buf[k] = d_buf[k] + rd[k] * natural(s1_full, k)
    ready_wait(0)
    ready_signal(1)
    phi(scaled)
    for k in range(OWN):
        d_buf[k] = d_buf[k] + rd[k] * natural(s2_full, k)
    gather_u.forward()
    phi(scaled)
    for k in range(OWN):
        d_buf[k] = d_buf[k] + rd[k] * natural(s3_own, k)
    ready_wait(1)
    ready_signal(2)

    def respond(z, x):
        v_buf[z] = x

    phi(respond)

    part_right = remote(v_buf.at[pl.ds(8, 2)], rs_left, rs_send.at[0], rs_recv.at[0], at(c, right))
    part_left = remote(v_buf.at[pl.ds(10, 2)], rs_right, rs_send.at[1], rs_recv.at[1], at(c, left))
    part_right.start()
    part_left.start()
    v_own = remote(v_buf.at[pl.ds(0, 4)], rv_own, v_send.at[0], v_recv.at[0], at(after, d))
    v_own.start()
    v_right_late = remote(v_buf.at[pl.ds(6, 2)], rv_left.at[pl.ds(2, 2)],
                          v_send.at[1], v_recv.at[1], at(after, right))
    v_left_late = remote(v_buf.at[pl.ds(12, 2)], rv_right.at[pl.ds(0, 2)],
                         v_send.at[2], v_recv.at[2], at(after, left))
    v_right_late.start()
    v_left_late.start()
    part_right.wait_recv()
    for k in range(2):
        v_buf[4 + k] = v_buf[4 + k] + rs_left[k]
    v_right = remote(v_buf.at[pl.ds(4, 2)], rv_left.at[pl.ds(0, 2)],
                     v_send.at[3], v_recv.at[3], at(after, right))
    v_right.start()
    part_left.wait_recv()
    for k in range(2):
        v_buf[14 + k] = v_buf[14 + k] + rs_right[k]
    v_left = remote(v_buf.at[pl.ds(14, 2)], rv_right.at[pl.ds(2, 2)],
                    v_send.at[4], v_recv.at[4], at(after, left))
    v_left.start()

    gather_u.finish()
    for z in range(NZ):
        d_buf[z] = rd[z] * natural(u_full, z)

    def first(z, x):
        x_buf[4, z] = x

    phi(first)
    ready_wait(2)
    ready_signal(3)

    for copy in (v_own, v_right_late, v_left_late, v_right, v_left):
        copy.wait_recv()
    has_before = jnp.where(c > 0, 1.0, 0.0).astype(jnp.float32)
    for k in range(OWN):
        q = has_before * (rv_own[k] + rv_left[k] + rv_right[k])
        point = q + natural(s0_own, k)
        put_natural(stage, point, 0, k)
        e_full[k] = point - natural(u_full, k)
    gather_e.start()
    outs = [pltpu.make_async_copy(stage.at[0], relaxed.at[0], out_sem.at[0])]
    outs[0].start()
    gather_e.forward()
    gather_s1.start()

    known = ALL - frozenset((8, 9, 10, 11))
    for z in known:
        d_buf[z] = rd[z] * e_full[z]
    inner = [known]
    for number in range(1, SWEEPS):
        inner.append(ALL - grow(ALL - inner[-1]))
        level(number, inner[number], ALL, ALL)
    gather_e.finish()
    for z in ALL - known:
        d_buf[z] = rd[z] * e_full[z]
    for number in range(1, SWEEPS):
        level(number, ALL - inner[number], ALL, ALL)

    def chain(j):
        def emit(z, x):
            x_buf[j, z] = x
            d_buf[z] = rd[z] * x
        return emit

    last_step(ALL, ALL, chain(0))
    phi(chain(1))
    gather_s1.forward()
    gather_s2.start()
    phi(chain(2))
    ready_wait(3)

    squares = []

    def last(z, x):
        if z < OWN:
            x_buf[3, z] = x
        squares.append(x * x)

    phi(last)
    total = squares[0]
    for square in squares[1:]:
        total = total + square
    has_after = jnp.where(c < tms - 1, 1.0, 0.0).astype(jnp.float32)
    na[0] = has_after * jnp.sum(jnp.sum(total, axis=0), axis=0, keepdims=True)
    na_copy = remote(na.at[0], na.at[1], na_send.at[0], na_recv.at[0], at(partner, d))
    na_copy.start()
    r_copy = remote(x_buf.at[3, pl.ds(0, 4)], r_recv, r_send.at[0], r_recv_sem.at[0], at(after, d))
    na_copy.wait_recv()
    nb[0] = na[0] + na[1]
    nb_copies = []
    for i in range(1, levels * COLUMNS):
        target = lax.rem(plane + i // COLUMNS, levels) * PLANE + lax.rem(seat + 2 * (i % COLUMNS), PLANE)
        copy = remote(nb.at[0], nb.at[i], nb_send.at[i - 1], nb_recv.at[i - 1], at(target, d))
        copy.start()
        nb_copies.append(copy)
    r_copy.start()

    gather_s2.forward()
    gather_s1.finish()
    for z in range(NZ):
        d_buf[z] = rd[z] * (x_buf[4, z] + natural(s1_full, z))
    for k in range(OWN):
        value = x_buf[4, k] + natural(s1_full, k) + x_buf[0, k]
        put_natural(stage, value, 1, k)
    outs.append(pltpu.make_async_copy(stage.at[1], relaxed.at[1], out_sem.at[1]))
    outs[1].start()
    near = frozenset(range(OWN))
    for _ in range(SWEEPS):
        near = grow(near)
    phi(first, near)
    gather_s2.finish()
    for z in near:
        d_buf[z] = rd[z] * (x_buf[4, z] + natural(s2_full, z))
    for k in range(OWN):
        value = x_buf[4, k] + natural(s2_full, k) + x_buf[1, k]
        put_natural(stage, value, 2, k)
    outs.append(pltpu.make_async_copy(stage.at[2], relaxed.at[2], out_sem.at[2]))
    outs[2].start()
    phi(first, range(OWN))
    for k in range(OWN):
        value = x_buf[4, k] + natural(s3_own, k) + x_buf[2, k]
        put_natural(stage, value, 3, k)
    outs.append(pltpu.make_async_copy(stage.at[3], relaxed.at[3], out_sem.at[3]))
    outs[3].start()

    r_copy.wait_recv()
    for k in range(OWN):
        put_natural(r_stage, has_before * r_recv[k], k)
    outs.append(pltpu.make_async_copy(r_stage, residual.at[0], out_sem.at[4]))
    outs[4].start()

    for copy in nb_copies:
        copy.wait_recv()
    row = nb[0]
    for i in range(1, levels * COLUMNS):
        row = row + nb[i]
    norm[...] = jnp.broadcast_to(jnp.sum(row, axis=1, keepdims=True), (1, NY))

    for gather in (gather_u, gather_s1, gather_s2, gather_e):
        gather.drain()
    for copy in (a_right, a_left, a_on_right, a_on_left, a_give_left, a_give_right, a_give_first, a_give_second):
        copy.wait_send()
    for copy in (part_right, part_left, v_own, v_right_late, v_left_late, v_right, v_left, r_copy, na_copy):
        copy.wait_send()
    for copy in nb_copies:
        copy.wait_send()
    for copy in outs:
        copy.wait()


def local(state, source, absorption):
    levels = lax.axis_size("tm") // PLANE
    f32 = jnp.float32
    packed = (NZ, 8, 8, NY)
    any_spec = pl.BlockSpec(memory_space=pl.ANY)
    vm = lambda *shape: pltpu.VMEM(shape, f32)
    dma = lambda *shape: pltpu.SemaphoreType.DMA(shape)
    relaxed, residual, norm = pl.pallas_call(
        kernel,
        out_shape=(
            jax.ShapeDtypeStruct((CF, OWN, NX, NY), f32),
            jax.ShapeDtypeStruct((1, OWN, NX, NY), f32),
            jax.ShapeDtypeStruct((1, NY), f32),
        ),
        in_specs=[any_spec] * 3,
        out_specs=(any_spec, any_spec, pl.BlockSpec(memory_space=pltpu.VMEM)),
        scratch_shapes=[
            vm(NZ, NX, NY), vm(NZ, NX, NY), vm(NZ, NX, NY), vm(NZ, NX, NY),
            vm(OWN, NX, NY), vm(OWN, NX, NY),
            vm(*packed), vm(*packed), vm(*packed), vm(*packed),
            vm(*packed), vm(*packed), vm(*packed), vm(*packed), vm(*packed),
            vm(*packed), vm(*packed), vm(5, *packed),
            vm(2, 8, 8, NY), vm(2, 8, 8, NY),
            vm(OWN, 8, 8, NY), vm(OWN, 8, 8, NY), vm(OWN, 8, 8, NY),
            vm(CF, OWN, NX, NY), vm(OWN, 8, 8, NY), vm(OWN, NX, NY),
            vm(2, 1, NY), vm(levels * COLUMNS, 1, NY),
            dma(6), dma(5), dma(8), dma(8), dma(4, 4), dma(4, 4), dma(2), dma(2), dma(5), dma(5),
            dma(1), dma(1), dma(1), dma(1), dma(levels * COLUMNS - 1), dma(levels * COLUMNS - 1),
            pltpu.SemaphoreType.REGULAR((len(REACHES),)),
        ],
        compiler_params=pltpu.CompilerParams(
            collective_id=0, has_side_effects=True, vmem_limit_bytes=VMEM_BYTES
        ),
    )(state, source, absorption)
    return relaxed, residual, norm[0, 0]


def solution(mesh):
    return jax.shard_map(
        local,
        mesh=mesh,
        in_specs=(P("tm", "space", None, None), P("tm", "space", None, None), P("space", None, None)),
        out_specs=(P("tm", "space", None, None), P("tm", "space", None, None), P()),
        check_vma=False,
    )
```

```python
import math

import jax
import jax.numpy as jnp
import numpy as np
from jax import lax
from jax.experimental import pallas as pl
from jax.experimental.pallas import tpu as pltpu
from jax.sharding import PartitionSpec as P

MESH = pl.DeviceIdType.MESH
CF = 4
SWEEPS = 5
COUPLING = 4.0
NZ, NX, NY = 16, 64, 128
OWN = 4
SPACES = 4
PLANE = 8
REACHES = (1, 2, 4, 1)
COLUMNS = 4
HALF = 64
ALL = frozenset(range(16))
VMEM_BYTES = 54272 * 1024


def sweep_weights(count):
    spread = 6.0 * COUPLING / (1.0 + 6.0 * COUPLING)
    return [
        1.0 / (1.0 + spread * math.cos(math.pi * (2 * k + 1) / (2 * count))) for k in range(count)
    ]


def coefficients():
    poly = np.zeros(SWEEPS + 1)
    poly[0] = 1.0
    for w in sweep_weights(SWEEPS):
        shifted = np.concatenate([[0.0], poly[:-1]])
        poly = (1.0 - w) * poly + w * shifted
        poly[0] += w
    return [float(c) for c in poly]


COEF = coefficients()
C2 = 0.5 * (COEF[2] + COEF[3])
C4 = 0.5 * (COEF[4] + COEF[5])


def grow(layers):
    return frozenset((z + step) % NZ for z in layers for step in (-1, 0, 1))


def kernel(
    state, source, absorption, relaxed, residual, norm,
    a_full, u_full, s1_full, s2_full, s0_own, s3_own,
    rd, q1, q2, q3, d_buf, l1, l2, l3, l4, v_buf, e_full, x_buf,
    loaded, rs_left, rs_right, rv_own, rv_left, rv_right, stage, r_recv, r_stage,
    na, nb,
    local_sem, out_sem, a_send, a_recv, ag_send, ag_recv, rs_send, rs_recv, v_send, v_recv,
    r_send, r_recv_sem, na_send, na_recv, nb_send, nb_recv, ready_sem,
):
    c = lax.axis_index("tm")
    d = lax.axis_index("space")
    tms = lax.axis_size("tm")
    levels = tms // PLANE
    after, before = lax.rem(c + 1, tms), lax.rem(c + tms - 1, tms)
    right, left = lax.rem(d + 1, SPACES), lax.rem(d + SPACES - 1, SPACES)
    plane, seat = c // PLANE, lax.rem(c, PLANE)
    core = lax.rem(c, 2)
    partner = c + 1 - 2 * core

    def at(t, s):
        return {"tm": t, "space": s}

    def seat_at(i):
        return plane * PLANE + lax.rem(seat + i, PLANE)

    def level_at(i):
        return lax.rem(plane + i, levels) * PLANE + seat

    def remote(src, dst, send, recv, target):
        return pltpu.make_async_remote_copy(
            src_ref=src, dst_ref=dst, send_sem=send, recv_sem=recv,
            device_id=target, device_id_type=MESH,
        )

    loads = []
    for i, (src, dst) in enumerate([
        (absorption, loaded.at[0]),
        (state.at[0], loaded.at[1]),
        (source.at[1], loaded.at[2]),
        (source.at[2], loaded.at[3]),
        (source.at[0], loaded.at[4]),
        (source.at[3], loaded.at[5]),
    ]):
        copy = pltpu.make_async_copy(src, dst, local_sem.at[i])
        copy.start()
        loads.append(copy)

    barrier = pltpu.get_barrier_semaphore()
    peers = [at(c, left), at(c, right)]
    peers += [at(t, s) for t in (after, before) for s in (d, left, right)]
    peers += [at(seat_at(i), d) for i in range(1, PLANE)]
    peers += [at(level_at(i), d) for i in (1, levels - 1)]
    for peer in peers:
        pl.semaphore_signal(barrier, inc=1, device_id=peer, device_id_type=MESH)

    rows = lax.broadcasted_iota(jnp.int32, (8, NY), 0)
    lane = lax.broadcasted_iota(jnp.int32, (8, NY), 1)
    lanes = lax.broadcasted_iota(jnp.int32, (4, 8, NY), 2) % HALF
    even, lower = lane % 2 == 0, lane < HALF
    split = 2 * (lane % HALF) + lane // HALF
    merge = HALF * (lane % 2) + lane // 2
    inner_up, inner_down = rows != 7, rows != 0
    edge_up, edge_down = (rows == 7) & (lane >= HALF), (rows == 0) & lower

    def pick(x, index):
        return jnp.take_along_axis(x, index, axis=1)
    joined = [jnp.where(d == SPACES - 1 - b, 0.0, 1.0).astype(jnp.float32) for b in range(SPACES)]

    def natural(ref, *index):
        tiles = [[], []]
        for w in range(4):
            top = ref[(*index, pl.ds(w, 8, stride=4), slice(None))]
            low = ref[(*index, pl.ds(NX // 2 + w, 8, stride=4), slice(None))]
            tiles[0].append(pick(jnp.where(even, top, pltpu.roll(low, 1, 1)), split))
            tiles[1].append(pick(jnp.where(even, pltpu.roll(top, NY - 1, 1), low), split))
        return jnp.stack(tiles[0] + tiles[1])

    def put_natural(ref, value, *index):
        for w in range(4):
            first, second = pick(value[w], merge), pick(value[4 + w], merge)
            ref[(*index, pl.ds(w, 8, stride=4), slice(None))] = jnp.where(even, first, pltpu.roll(second, 1, 1))
            ref[(*index, pl.ds(NX // 2 + w, 8, stride=4), slice(None))] = jnp.where(even, pltpu.roll(first, NY - 1, 1), second)

    def ready_signal(number):
        reach = REACHES[number]
        for i in (reach, levels - reach):
            pl.semaphore_signal(ready_sem.at[number], inc=1, device_id=at(level_at(i), d), device_id_type=MESH)

    def ready_wait(number):
        pl.semaphore_wait(ready_sem.at[number], 2)

    class Gather:
        def __init__(self, full, slot):
            self.full, self.slot = full, slot

        def copy(self, src, dst, count, part, target):
            return remote(self.full.at[pl.ds(src, count)], self.full.at[pl.ds(dst, count)],
                          ag_send.at[self.slot, part], ag_recv.at[self.slot, part], at(c, target))

        def start(self):
            self.first = [self.copy(0, 12, 1, 0, right), self.copy(3, 7, 1, 1, left),
                          self.copy(1, 13, 1, 2, right), self.copy(2, 6, 1, 3, left)]
            self.rest = [self.copy(2, 14, 2, 4, right), self.copy(0, 4, 2, 5, left)]
            self.onward = [self.copy(12, 8, 1, 6, right), self.copy(7, 11, 1, 7, left),
                           self.copy(13, 9, 1, 8, right), self.copy(6, 10, 1, 9, left)]
            for copy in self.first + self.rest:
                copy.start()

        def forward(self):
            for came, goes in zip(self.first, self.onward):
                came.wait_recv()
                goes.start()

        def middle(self):
            for copy in self.rest:
                copy.wait_recv()

        def finish(self):
            for copy in self.onward:
                copy.wait_recv()

        def drain(self):
            for copy in self.first + self.rest + self.onward:
                copy.wait_send()

    gather_u, gather_s1, gather_s2 = Gather(u_full, 0), Gather(s1_full, 1), Gather(s2_full, 2)
    gather_e = Gather(e_full, 3)

    half = 2 * core

    def a_copy(src, dst, count, part, target):
        return remote(a_full.at[pl.ds(src, count)], a_full.at[pl.ds(dst, count)],
                      a_send.at[part], a_recv.at[part], target)

    a_right = a_copy(half, 12 + half, 1, 0, at(c, right))
    a_left = a_copy(half + 1, 4 + half + 1, 1, 1, at(c, left))
    a_right_rest = a_copy(half + 1, 12 + half + 1, 1, 8, at(c, right))
    a_left_rest = a_copy(half, 4 + half, 1, 9, at(c, left))
    a_on_right = a_copy(12 + half, 8 + half, 1, 2, at(c, right))
    a_on_left = a_copy(4 + half + 1, 8 + half + 1, 1, 3, at(c, left))
    a_give_left = a_copy(12 + half, 12 + half, 2, 4, at(partner, d))
    a_give_right = a_copy(4 + half, 4 + half, 2, 5, at(partner, d))
    a_give_first = a_copy(8 + half, 8 + half, 1, 6, at(partner, d))
    a_give_second = a_copy(8 + half + 1, 8 + half + 1, 1, 7, at(partner, d))

    def neighbours(ref, z, have):
        terms = []
        if z in have:
            x = ref[z]
            after_x, before_x = [], []
            for p in range(2):
                up, down = pltpu.roll(x[4 * p], 7, 0), pltpu.roll(x[4 * p + 3], 1, 0)
                across = pltpu.roll(jnp.where(edge_up, up, jnp.where(edge_down, down, 0.0)), HALF, 1)
                up = jnp.where(inner_up, up, across)
                down = jnp.where(inner_down, down, across)
                after_x += [x[4 * p + 1:4 * p + 4], up[None]]
                before_x += [down[None], x[4 * p:4 * p + 3]]
            terms.append(jnp.concatenate(after_x) + jnp.concatenate(before_x))
            evens, odds = x[:4], x[4:]
            terms.append(jnp.concatenate([odds, evens]))
            terms.append(jnp.concatenate([
                jnp.where(lanes == 0, 0.0, pltpu.roll(odds, 1, 2)),
                jnp.where(lanes == HALF - 1, 0.0, pltpu.roll(evens, NY - 1, 2)),
            ]))
        above, below = (z + 1) % NZ, (z - 1) % NZ
        if above in have:
            terms.append(ref[above] if above % OWN else joined[z // OWN] * ref[above])
        if below in have:
            terms.append(ref[below] if z % OWN else joined[below // OWN] * ref[below])
        total = terms[0]
        for term in terms[1:]:
            total = total + term
        return total

    steps = [(d_buf, l1, q1), (l1, l2, q2), (l2, l3, q1), (l3, l4, q3)]

    turn = [0]

    def in_turn(layers):
        turn[0] += 1
        return sorted(layers, key=lambda z: (z - turn[0]) % NZ)

    def level(number, layers, have, have_d):
        src, dst, factor = steps[number - 1]
        for z in in_turn(layers):
            value = factor[z] * neighbours(src, z, have)
            if number % 2 == 0 and z in have_d:
                value = d_buf[z] + value
            dst[z] = value

    def last_step(layers, have, emit):
        for z in in_turn(layers):
            value = q1[z] * neighbours(l4, z, have)
            emit(z, l4[z] + value if z in have else value)

    def phi(emit, want=ALL):
        need = [frozenset(want)]
        for _ in range(SWEEPS - 1):
            need.insert(0, grow(need[0]))
        for number in range(1, SWEEPS):
            level(number, need[number - 1], ALL, ALL)
        last_step(want, ALL, emit)

    def invert(layers):
        for z in layers:
            inverse = 1.0 / (1.0 + 6.0 * COUPLING + a_full[z])
            rd[z] = inverse
            q1[z] = COUPLING * inverse
            q2[z] = (COUPLING * C4 / C2) * inverse
            q3[z] = (COUPLING * C2) * inverse

    def place(full, number):
        loads[number].wait()
        for k in range(OWN):
            full[k] = natural(loaded, number, k)

    place(a_full, 0)
    pl.semaphore_wait(barrier, len(peers))

    a_right.start()
    a_left.start()
    a_right_rest.start()
    a_left_rest.start()
    ready_signal(0)
    invert(range(4))
    for full, number in ((u_full, 1), (s1_full, 2), (s2_full, 3), (s0_own, 4), (s3_own, 5)):
        place(full, number)
    for k in range(OWN):
        d_buf[k] = rd[k] * u_full[k]
    a_right.wait_recv()
    a_on_right.start()
    a_left.wait_recv()
    a_on_left.start()
    a_right_rest.wait_recv()
    a_give_left.start()
    a_left_rest.wait_recv()
    a_give_right.start()
    gather_u.start()
    a_give_left.wait_recv()
    a_give_right.wait_recv()
    invert((4, 5, 6, 7, 12, 13, 14, 15))

    reach = [frozenset(range(OWN))]
    for _ in range(SWEEPS):
        reach.append(grow(reach[-1]))
    for number in range(1, SWEEPS):
        level(number, reach[number], reach[number - 1], reach[0])
    a_on_right.wait_recv()
    a_give_first.start()
    a_on_left.wait_recv()
    a_give_second.start()
    a_give_first.wait_recv()
    a_give_second.wait_recv()
    invert((8, 9, 10, 11))
    for z in ALL - reach[SWEEPS]:
        d_buf[z] = jnp.zeros((8, 8, NY), jnp.float32)

    def scaled(z, x):
        d_buf[z] = rd[z] * x

    last_step(reach[SWEEPS], reach[SWEEPS - 1], scaled)
    for k in range(OWN):
        d_buf[k] = d_buf[k] + rd[k] * s1_full[k]
    ready_wait(0)
    ready_signal(1)
    phi(scaled)
    for k in range(OWN):
        d_buf[k] = d_buf[k] + rd[k] * s2_full[k]
    gather_u.forward()
    phi(scaled)
    for k in range(OWN):
        d_buf[k] = d_buf[k] + rd[k] * s3_own[k]
    ready_wait(1)
    ready_signal(2)

    def respond(z, x):
        v_buf[z] = x

    phi(respond)

    parts = []
    for k in range(2):
        parts.append((remote(v_buf.at[pl.ds(8 + k, 1)], rs_left.at[pl.ds(k, 1)],
                             rs_send.at[2 * k], rs_recv.at[2 * k], at(c, right)), 4 + k, rs_left, k))
        parts.append((remote(v_buf.at[pl.ds(10 + k, 1)], rs_right.at[pl.ds(k, 1)],
                             rs_send.at[2 * k + 1], rs_recv.at[2 * k + 1], at(c, left)), 14 + k, rs_right, k))
    for part in parts:
        part[0].start()
    v_copies = [
        remote(v_buf.at[pl.ds(0, 4)], rv_own, v_send.at[0], v_recv.at[0], at(after, d)),
        remote(v_buf.at[pl.ds(6, 2)], rv_left.at[pl.ds(2, 2)], v_send.at[1], v_recv.at[1], at(after, right)),
        remote(v_buf.at[pl.ds(12, 2)], rv_right.at[pl.ds(0, 2)], v_send.at[2], v_recv.at[2], at(after, left)),
    ]
    for copy in v_copies:
        copy.start()
    for i, (part, layer, came, k) in enumerate(parts):
        part.wait_recv()
        v_buf[layer] = v_buf[layer] + came[k]
        dst, target = (rv_left, right) if came is rs_left else (rv_right, left)
        copy = remote(v_buf.at[pl.ds(layer, 1)], dst.at[pl.ds(layer - (4 if came is rs_left else 12), 1)],
                      v_send.at[3 + i], v_recv.at[3 + i], at(after, target))
        copy.start()
        v_copies.append(copy)

    gather_u.middle()
    gather_u.finish()
    for z in range(NZ):
        d_buf[z] = rd[z] * u_full[z]

    def first(z, x):
        x_buf[4, z] = x

    phi(first)
    ready_wait(2)
    ready_signal(3)

    for copy in v_copies:
        copy.wait_recv()
    has_before = jnp.where(c > 0, 1.0, 0.0).astype(jnp.float32)
    for k in range(OWN):
        q = has_before * (rv_own[k] + rv_left[k] + rv_right[k])
        point = q + s0_own[k]
        put_natural(stage, point, 0, k)
        e_full[k] = point - u_full[k]
    gather_e.start()
    outs = [pltpu.make_async_copy(stage.at[0], relaxed.at[0], out_sem.at[0])]
    outs[0].start()
    gather_e.forward()
    gather_s1.start()
    gather_e.middle()

    known = ALL - frozenset((8, 9, 10, 11))
    for z in known:
        d_buf[z] = rd[z] * e_full[z]
    inner = [known]
    for number in range(1, SWEEPS):
        inner.append(ALL - grow(ALL - inner[-1]))
        level(number, inner[number], ALL, ALL)
    gather_e.finish()
    for z in ALL - known:
        d_buf[z] = rd[z] * e_full[z]
    for number in range(1, SWEEPS):
        level(number, ALL - inner[number], ALL, ALL)

    def chain(j):
        def emit(z, x):
            x_buf[j, z] = x
            d_buf[z] = rd[z] * x
        return emit

    last_step(ALL, ALL, chain(0))
    phi(chain(1))
    gather_s1.forward()
    gather_s2.start()
    phi(chain(2))
    ready_wait(3)

    squares = []

    def last(z, x):
        if z < OWN:
            x_buf[3, z] = x
        squares.append(x * x)

    phi(last)
    total = squares[0]
    for square in squares[1:]:
        total = total + square
    has_after = jnp.where(c < tms - 1, 1.0, 0.0).astype(jnp.float32)
    na[0] = has_after * jnp.sum(jnp.sum(total, axis=0), axis=0, keepdims=True)
    na_copy = remote(na.at[0], na.at[1], na_send.at[0], na_recv.at[0], at(partner, d))
    na_copy.start()
    r_copy = remote(x_buf.at[3, pl.ds(0, 4)], r_recv, r_send.at[0], r_recv_sem.at[0], at(after, d))
    na_copy.wait_recv()
    nb[0] = na[0] + na[1]
    nb_copies = []
    for i in range(1, levels * COLUMNS):
        target = lax.rem(plane + i // COLUMNS, levels) * PLANE + lax.rem(seat + 2 * (i % COLUMNS), PLANE)
        copy = remote(nb.at[0], nb.at[i], nb_send.at[i - 1], nb_recv.at[i - 1], at(target, d))
        copy.start()
        nb_copies.append(copy)
    r_copy.start()

    gather_s2.forward()
    gather_s1.middle()
    gather_s1.finish()
    for z in range(NZ):
        d_buf[z] = rd[z] * (x_buf[4, z] + s1_full[z])
    for k in range(OWN):
        value = x_buf[4, k] + s1_full[k] + x_buf[0, k]
        put_natural(stage, value, 1, k)
    outs.append(pltpu.make_async_copy(stage.at[1], relaxed.at[1], out_sem.at[1]))
    outs[1].start()
    near = frozenset(range(OWN))
    for _ in range(SWEEPS):
        near = grow(near)
    phi(first, near)
    gather_s2.middle()
    gather_s2.finish()
    for z in near:
        d_buf[z] = rd[z] * (x_buf[4, z] + s2_full[z])
    for k in range(OWN):
        value = x_buf[4, k] + s2_full[k] + x_buf[1, k]
        put_natural(stage, value, 2, k)
    outs.append(pltpu.make_async_copy(stage.at[2], relaxed.at[2], out_sem.at[2]))
    outs[2].start()
    phi(first, range(OWN))
    for k in range(OWN):
        value = x_buf[4, k] + s3_own[k] + x_buf[2, k]
        put_natural(stage, value, 3, k)
    outs.append(pltpu.make_async_copy(stage.at[3], relaxed.at[3], out_sem.at[3]))
    outs[3].start()

    r_copy.wait_recv()
    for k in range(OWN):
        put_natural(r_stage, has_before * r_recv[k], k)
    outs.append(pltpu.make_async_copy(r_stage, residual.at[0], out_sem.at[4]))
    outs[4].start()

    for copy in nb_copies:
        copy.wait_recv()
    row = nb[0]
    for i in range(1, levels * COLUMNS):
        row = row + nb[i]
    norm[...] = jnp.broadcast_to(jnp.sum(row, axis=1, keepdims=True), (1, NY))

    for gather in (gather_u, gather_s1, gather_s2, gather_e):
        gather.drain()
    for copy in (a_right_rest, a_left_rest, a_right, a_left, a_on_right, a_on_left, a_give_left, a_give_right, a_give_first, a_give_second):
        copy.wait_send()
    for copy in [part[0] for part in parts] + v_copies + [r_copy, na_copy]:
        copy.wait_send()
    for copy in nb_copies:
        copy.wait_send()
    for copy in outs:
        copy.wait()


def local(state, source, absorption):
    levels = lax.axis_size("tm") // PLANE
    f32 = jnp.float32
    packed = (NZ, 8, 8, NY)
    any_spec = pl.BlockSpec(memory_space=pl.ANY)
    vm = lambda *shape: pltpu.VMEM(shape, f32)
    dma = lambda *shape: pltpu.SemaphoreType.DMA(shape)
    relaxed, residual, norm = pl.pallas_call(
        kernel,
        out_shape=(
            jax.ShapeDtypeStruct((CF, OWN, NX, NY), f32),
            jax.ShapeDtypeStruct((1, OWN, NX, NY), f32),
            jax.ShapeDtypeStruct((1, NY), f32),
        ),
        in_specs=[any_spec] * 3,
        out_specs=(any_spec, any_spec, pl.BlockSpec(memory_space=pltpu.VMEM)),
        scratch_shapes=[
            vm(*packed), vm(*packed), vm(*packed), vm(*packed),
            vm(OWN, 8, 8, NY), vm(OWN, 8, 8, NY),
            vm(*packed), vm(*packed), vm(*packed), vm(*packed),
            vm(*packed), vm(*packed), vm(*packed), vm(*packed), vm(*packed),
            vm(*packed), vm(*packed), vm(5, *packed),
            vm(6, OWN, NX, NY), vm(2, 8, 8, NY), vm(2, 8, 8, NY),
            vm(OWN, 8, 8, NY), vm(OWN, 8, 8, NY), vm(OWN, 8, 8, NY),
            vm(CF, OWN, NX, NY), vm(OWN, 8, 8, NY), vm(OWN, NX, NY),
            vm(2, 1, NY), vm(levels * COLUMNS, 1, NY),
            dma(6), dma(5), dma(10), dma(10), dma(4, 10), dma(4, 10), dma(4), dma(4), dma(7), dma(7),
            dma(1), dma(1), dma(1), dma(1), dma(levels * COLUMNS - 1), dma(levels * COLUMNS - 1),
            pltpu.SemaphoreType.REGULAR((len(REACHES),)),
        ],
        compiler_params=pltpu.CompilerParams(
            collective_id=0, has_side_effects=True, vmem_limit_bytes=VMEM_BYTES
        ),
    )(state, source, absorption)
    return relaxed, residual, norm[0, 0]


def solution(mesh):
    return jax.shard_map(
        local,
        mesh=mesh,
        in_specs=(P("tm", "space", None, None), P("tm", "space", None, None), P("space", None, None)),
        out_specs=(P("tm", "space", None, None), P("tm", "space", None, None), P()),
        check_vma=False,
    )
```

```python
import math

import jax
import jax.numpy as jnp
import numpy as np
from jax import lax
from jax.experimental import pallas as pl
from jax.experimental.pallas import tpu as pltpu
from jax.sharding import PartitionSpec as P

MESH = pl.DeviceIdType.MESH
CF = 4
SWEEPS = 5
COUPLING = 4.0
NZ, NX, NY = 16, 64, 128
OWN = 4
SPACES = 4
PLANE = 8
REACHES = (1, 2, 4, 1)
COLUMNS = 4
HALF = 64
ALL = frozenset(range(16))
VMEM_BYTES = 48 * 1024 * 1024


def sweep_weights(count):
    spread = 6.0 * COUPLING / (1.0 + 6.0 * COUPLING)
    return [
        1.0 / (1.0 + spread * math.cos(math.pi * (2 * k + 1) / (2 * count))) for k in range(count)
    ]


def coefficients():
    poly = np.zeros(SWEEPS + 1)
    poly[0] = 1.0
    for w in sweep_weights(SWEEPS):
        shifted = np.concatenate([[0.0], poly[:-1]])
        poly = (1.0 - w) * poly + w * shifted
        poly[0] += w
    return [float(c) for c in poly]


COEF = coefficients()
C2 = 0.5 * (COEF[2] + COEF[3])
C4 = 0.5 * (COEF[4] + COEF[5])


def grow(layers):
    return frozenset((z + step) % NZ for z in layers for step in (-1, 0, 1))


def kernel(
    state, source, absorption, relaxed, residual, norm,
    a_full, u_full, s1_full, s2_full, s0_own, s3_own,
    rd, q1, q2, q3, d_buf, l1, l2, l3, l4, v_buf, e_full, x_buf,
    loaded, rs_left, rs_right, rv_own, rv_left, rv_right, stage, r_recv, r_stage,
    na, nb,
    local_sem, out_sem, a_send, a_recv, ag_send, ag_recv, rs_send, rs_recv, v_send, v_recv,
    r_send, r_recv_sem, na_send, na_recv, nb_send, nb_recv, ready_sem,
):
    c = lax.axis_index("tm")
    d = lax.axis_index("space")
    tms = lax.axis_size("tm")
    levels = tms // PLANE
    after, before = lax.rem(c + 1, tms), lax.rem(c + tms - 1, tms)
    right, left = lax.rem(d + 1, SPACES), lax.rem(d + SPACES - 1, SPACES)
    plane, seat = c // PLANE, lax.rem(c, PLANE)
    core = lax.rem(c, 2)
    partner = c + 1 - 2 * core

    def at(t, s):
        return {"tm": t, "space": s}

    def seat_at(i):
        return plane * PLANE + lax.rem(seat + i, PLANE)

    def level_at(i):
        return lax.rem(plane + i, levels) * PLANE + seat

    def remote(src, dst, send, recv, target):
        return pltpu.make_async_remote_copy(
            src_ref=src, dst_ref=dst, send_sem=send, recv_sem=recv,
            device_id=target, device_id_type=MESH,
        )

    loads = []
    for i, (src, dst) in enumerate([
        (absorption, loaded.at[0]),
        (state.at[0], loaded.at[1]),
        (source.at[1], loaded.at[2]),
        (source.at[2], loaded.at[3]),
        (source.at[0], loaded.at[4]),
        (source.at[3], loaded.at[5]),
    ]):
        copy = pltpu.make_async_copy(src, dst, local_sem.at[i])
        copy.start()
        loads.append(copy)

    barrier = pltpu.get_barrier_semaphore()
    peers = [at(c, left), at(c, right)]
    peers += [at(t, s) for t in (after, before) for s in (d, left, right)]
    peers += [at(seat_at(i), d) for i in range(1, PLANE)]
    peers += [at(level_at(i), d) for i in (1, levels - 1)]
    for peer in peers:
        pl.semaphore_signal(barrier, inc=1, device_id=peer, device_id_type=MESH)

    rows = lax.broadcasted_iota(jnp.int32, (8, NY), 0)
    lane = lax.broadcasted_iota(jnp.int32, (8, NY), 1)
    lanes = lax.broadcasted_iota(jnp.int32, (4, 8, NY), 2) % HALF
    even, lower = lane % 2 == 0, lane < HALF
    split = 2 * (lane % HALF) + lane // HALF
    merge = HALF * (lane % 2) + lane // 2
    inner_up, inner_down = rows != 7, rows != 0
    edge_up, edge_down = (rows == 7) & (lane >= HALF), (rows == 0) & lower

    def pick(x, index):
        return jnp.take_along_axis(x, index, axis=1)
    joined = [jnp.where(d == SPACES - 1 - b, 0.0, 1.0).astype(jnp.float32) for b in range(SPACES)]

    def natural(ref, *index):
        tiles = [[], []]
        for w in range(4):
            top = ref[(*index, pl.ds(w, 8, stride=4), slice(None))]
            low = ref[(*index, pl.ds(NX // 2 + w, 8, stride=4), slice(None))]
            tiles[0].append(pick(jnp.where(even, top, pltpu.roll(low, 1, 1)), split))
            tiles[1].append(pick(jnp.where(even, pltpu.roll(top, NY - 1, 1), low), split))
        return jnp.stack(tiles[0] + tiles[1])

    def put_natural(ref, value, *index):
        for w in range(4):
            first, second = pick(value[w], merge), pick(value[4 + w], merge)
            ref[(*index, pl.ds(w, 8, stride=4), slice(None))] = jnp.where(even, first, pltpu.roll(second, 1, 1))
            ref[(*index, pl.ds(NX // 2 + w, 8, stride=4), slice(None))] = jnp.where(even, pltpu.roll(first, NY - 1, 1), second)

    def ready_signal(number):
        reach = REACHES[number]
        for i in (reach, levels - reach):
            pl.semaphore_signal(ready_sem.at[number], inc=1, device_id=at(level_at(i), d), device_id_type=MESH)

    def ready_wait(number):
        pl.semaphore_wait(ready_sem.at[number], 2)

    class Gather:
        def __init__(self, full, slot):
            self.full, self.slot = full, slot

        def copy(self, src, dst, count, part, target):
            return remote(self.full.at[pl.ds(src, count)], self.full.at[pl.ds(dst, count)],
                          ag_send.at[self.slot, part], ag_recv.at[self.slot, part], at(c, target))

        def start(self):
            self.first = [self.copy(0, 12, 1, 0, right), self.copy(3, 7, 1, 1, left),
                          self.copy(1, 13, 1, 2, right), self.copy(2, 6, 1, 3, left)]
            self.rest = [self.copy(2, 14, 2, 4, right), self.copy(0, 4, 2, 5, left)]
            self.onward = [self.copy(12, 8, 1, 6, right), self.copy(7, 11, 1, 7, left),
                           self.copy(13, 9, 1, 8, right), self.copy(6, 10, 1, 9, left)]
            for copy in self.first + self.rest:
                copy.start()

        def forward(self):
            for came, goes in zip(self.first, self.onward):
                came.wait_recv()
                goes.start()

        def middle(self):
            for copy in self.rest:
                copy.wait_recv()

        def finish(self):
            for copy in self.onward:
                copy.wait_recv()

        def drain(self):
            for copy in self.first + self.rest + self.onward:
                copy.wait_send()

    gather_u, gather_s1, gather_s2 = Gather(u_full, 0), Gather(s1_full, 1), Gather(s2_full, 2)
    gather_e = Gather(e_full, 3)

    half = 2 * core

    def a_copy(src, dst, count, part, target):
        return remote(a_full.at[pl.ds(src, count)], a_full.at[pl.ds(dst, count)],
                      a_send.at[part], a_recv.at[part], target)

    a_right = a_copy(half, 12 + half, 1, 0, at(c, right))
    a_left = a_copy(half + 1, 4 + half + 1, 1, 1, at(c, left))
    a_right_rest = a_copy(half + 1, 12 + half + 1, 1, 8, at(c, right))
    a_left_rest = a_copy(half, 4 + half, 1, 9, at(c, left))
    a_on_right = a_copy(12 + half, 8 + half, 1, 2, at(c, right))
    a_on_left = a_copy(4 + half + 1, 8 + half + 1, 1, 3, at(c, left))
    a_give_left = a_copy(12 + half, 12 + half, 2, 4, at(partner, d))
    a_give_right = a_copy(4 + half, 4 + half, 2, 5, at(partner, d))
    a_give_first = a_copy(8 + half, 8 + half, 1, 6, at(partner, d))
    a_give_second = a_copy(8 + half + 1, 8 + half + 1, 1, 7, at(partner, d))

    def neighbours(ref, z, have):
        terms = []
        if z in have:
            x = ref[z]
            after_x, before_x = [], []
            for p in range(2):
                up, down = pltpu.roll(x[4 * p], 7, 0), pltpu.roll(x[4 * p + 3], 1, 0)
                across = pltpu.roll(jnp.where(edge_up, up, jnp.where(edge_down, down, 0.0)), HALF, 1)
                up = jnp.where(inner_up, up, across)
                down = jnp.where(inner_down, down, across)
                after_x += [x[4 * p + 1:4 * p + 4], up[None]]
                before_x += [down[None], x[4 * p:4 * p + 3]]
            terms.append(jnp.concatenate(after_x) + jnp.concatenate(before_x))
            evens, odds = x[:4], x[4:]
            terms.append(jnp.concatenate([odds, evens]))
            terms.append(jnp.concatenate([
                jnp.where(lanes == 0, 0.0, pltpu.roll(odds, 1, 2)),
                jnp.where(lanes == HALF - 1, 0.0, pltpu.roll(evens, NY - 1, 2)),
            ]))
        above, below = (z + 1) % NZ, (z - 1) % NZ
        if above in have:
            terms.append(ref[above] if above % OWN else joined[z // OWN] * ref[above])
        if below in have:
            terms.append(ref[below] if z % OWN else joined[below // OWN] * ref[below])
        total = terms[0]
        for term in terms[1:]:
            total = total + term
        return total

    steps = [(d_buf, l1, q1), (l1, l2, q2), (l2, l3, q1), (l3, l4, q3)]

    turn = [0]

    def in_turn(layers):
        turn[0] += 1
        return sorted(layers, key=lambda z: (z - turn[0]) % NZ)

    def level(number, layers, have, have_d):
        src, dst, factor = steps[number - 1]
        for z in in_turn(layers):
            value = factor[z] * neighbours(src, z, have)
            if number % 2 == 0 and z in have_d:
                value = d_buf[z] + value
            dst[z] = value

    def last_step(layers, have, emit, order=None):
        for z in order or in_turn(layers):
            value = q1[z] * neighbours(l4, z, have)
            emit(z, l4[z] + value if z in have else value)

    def phi(emit, want=ALL, order=None):
        need = [frozenset(want)]
        for _ in range(SWEEPS - 1):
            need.insert(0, grow(need[0]))
        for number in range(1, SWEEPS):
            level(number, need[number - 1], ALL, ALL)
        last_step(want, ALL, emit, order)

    def invert(layers):
        for z in layers:
            inverse = 1.0 / (1.0 + 6.0 * COUPLING + a_full[z])
            rd[z] = inverse
            q1[z] = COUPLING * inverse
            q2[z] = (COUPLING * C4 / C2) * inverse
            q3[z] = (COUPLING * C2) * inverse

    def place(full, number):
        loads[number].wait()
        for k in range(OWN):
            full[k] = natural(loaded, number, k)

    place(a_full, 0)
    pl.semaphore_wait(barrier, len(peers))

    a_right.start()
    a_left.start()
    a_right_rest.start()
    a_left_rest.start()
    ready_signal(0)
    invert(range(4))
    for full, number in ((u_full, 1), (s1_full, 2), (s2_full, 3), (s0_own, 4), (s3_own, 5)):
        place(full, number)
    for k in range(OWN):
        d_buf[k] = rd[k] * u_full[k]
    a_right.wait_recv()
    a_on_right.start()
    a_left.wait_recv()
    a_on_left.start()
    a_right_rest.wait_recv()
    a_give_left.start()
    a_left_rest.wait_recv()
    a_give_right.start()
    gather_u.start()
    a_give_left.wait_recv()
    a_give_right.wait_recv()
    invert((4, 5, 6, 7, 12, 13, 14, 15))

    reach = [frozenset(range(OWN))]
    for _ in range(SWEEPS):
        reach.append(grow(reach[-1]))
    for number in range(1, SWEEPS):
        level(number, reach[number], reach[number - 1], reach[0])
    a_on_right.wait_recv()
    a_give_first.start()
    a_on_left.wait_recv()
    a_give_second.start()
    a_give_first.wait_recv()
    a_give_second.wait_recv()
    invert((8, 9, 10, 11))
    for z in ALL - reach[SWEEPS]:
        d_buf[z] = jnp.zeros((8, 8, NY), jnp.float32)

    def scaled(z, x):
        d_buf[z] = rd[z] * x

    last_step(reach[SWEEPS], reach[SWEEPS - 1], scaled)
    for k in range(OWN):
        d_buf[k] = d_buf[k] + rd[k] * s1_full[k]
    ready_wait(0)
    ready_signal(1)
    phi(scaled)
    for k in range(OWN):
        d_buf[k] = d_buf[k] + rd[k] * s2_full[k]
    gather_u.forward()
    phi(scaled)
    for k in range(OWN):
        d_buf[k] = d_buf[k] + rd[k] * s3_own[k]
    ready_wait(1)
    ready_signal(2)

    parts = []
    for k in range(2):
        parts.append((remote(v_buf.at[pl.ds(8 + k, 1)], rs_left.at[pl.ds(k, 1)],
                             rs_send.at[2 * k], rs_recv.at[2 * k], at(c, right)), 4 + k, rs_left, k))
        parts.append((remote(v_buf.at[pl.ds(10 + k, 1)], rs_right.at[pl.ds(k, 1)],
                             rs_send.at[2 * k + 1], rs_recv.at[2 * k + 1], at(c, left)), 14 + k, rs_right, k))

    def respond(z, x):
        v_buf[z] = x
        if z == 11:
            for part in parts:
                part[0].start()

    phi(respond, ALL, (8, 9, 10, 11, 6, 7, 12, 13, 0, 1, 2, 3, 4, 5, 14, 15))
    v_copies = [
        remote(v_buf.at[pl.ds(0, 4)], rv_own, v_send.at[0], v_recv.at[0], at(after, d)),
        remote(v_buf.at[pl.ds(6, 2)], rv_left.at[pl.ds(2, 2)], v_send.at[1], v_recv.at[1], at(after, right)),
        remote(v_buf.at[pl.ds(12, 2)], rv_right.at[pl.ds(0, 2)], v_send.at[2], v_recv.at[2], at(after, left)),
    ]
    for copy in v_copies:
        copy.start()
    for i, (part, layer, came, k) in enumerate(parts):
        part.wait_recv()
        v_buf[layer] = v_buf[layer] + came[k]
        dst, target = (rv_left, right) if came is rs_left else (rv_right, left)
        copy = remote(v_buf.at[pl.ds(layer, 1)], dst.at[pl.ds(layer - (4 if came is rs_left else 12), 1)],
                      v_send.at[3 + i], v_recv.at[3 + i], at(after, target))
        copy.start()
        v_copies.append(copy)

    gather_u.middle()
    gather_u.finish()
    for z in range(NZ):
        d_buf[z] = rd[z] * u_full[z]

    def first(z, x):
        x_buf[4, z] = x

    phi(first)
    ready_wait(2)
    ready_signal(3)

    for copy in v_copies:
        copy.wait_recv()
    has_before = jnp.where(c > 0, 1.0, 0.0).astype(jnp.float32)
    for k in range(OWN):
        q = has_before * (rv_own[k] + rv_left[k] + rv_right[k])
        e_full[k] = q + s0_own[k] - u_full[k]
    gather_e.start()
    for k in range(OWN):
        q = has_before * (rv_own[k] + rv_left[k] + rv_right[k])
        put_natural(stage, q + s0_own[k], 0, k)
    outs = [pltpu.make_async_copy(stage.at[0], relaxed.at[0], out_sem.at[0])]
    outs[0].start()
    gather_e.forward()
    gather_s1.start()
    gather_e.middle()

    known = ALL - frozenset((8, 9, 10, 11))
    for z in known:
        d_buf[z] = rd[z] * e_full[z]
    inner = [known]
    for number in range(1, SWEEPS):
        inner.append(ALL - grow(ALL - inner[-1]))
        level(number, inner[number], ALL, ALL)
    gather_e.finish()
    for z in ALL - known:
        d_buf[z] = rd[z] * e_full[z]
    for number in range(1, SWEEPS):
        level(number, ALL - inner[number], ALL, ALL)

    def chain(j):
        def emit(z, x):
            x_buf[j, z] = x
            d_buf[z] = rd[z] * x
        return emit

    last_step(ALL, ALL, chain(0))
    phi(chain(1))
    gather_s1.forward()
    gather_s2.start()
    phi(chain(2))
    ready_wait(3)

    squares = []

    def last(z, x):
        if z < OWN:
            x_buf[3, z] = x
        squares.append(x * x)

    phi(last)
    total = squares[0]
    for square in squares[1:]:
        total = total + square
    has_after = jnp.where(c < tms - 1, 1.0, 0.0).astype(jnp.float32)
    na[0] = has_after * jnp.sum(jnp.sum(total, axis=0), axis=0, keepdims=True)
    na_copy = remote(na.at[0], na.at[1], na_send.at[0], na_recv.at[0], at(partner, d))
    na_copy.start()
    r_copy = remote(x_buf.at[3, pl.ds(0, 4)], r_recv, r_send.at[0], r_recv_sem.at[0], at(after, d))
    na_copy.wait_recv()
    nb[0] = na[0] + na[1]
    nb_copies = []
    farthest_first = sorted(range(1, levels * COLUMNS), key=lambda i: -min(i // COLUMNS, levels - i // COLUMNS))
    for i in farthest_first:
        target = lax.rem(plane + i // COLUMNS, levels) * PLANE + lax.rem(seat + 2 * (i % COLUMNS), PLANE)
        copy = remote(nb.at[0], nb.at[i], nb_send.at[i - 1], nb_recv.at[i - 1], at(target, d))
        copy.start()
        nb_copies.append(copy)
    r_copy.start()

    gather_s2.forward()
    gather_s1.middle()
    gather_s1.finish()
    for z in range(NZ):
        d_buf[z] = rd[z] * (x_buf[4, z] + s1_full[z])
    for k in range(OWN):
        value = x_buf[4, k] + s1_full[k] + x_buf[0, k]
        put_natural(stage, value, 1, k)
    outs.append(pltpu.make_async_copy(stage.at[1], relaxed.at[1], out_sem.at[1]))
    outs[1].start()
    near = frozenset(range(OWN))
    for _ in range(SWEEPS):
        near = grow(near)
    phi(first, near)
    gather_s2.middle()
    gather_s2.finish()
    for z in near:
        d_buf[z] = rd[z] * (x_buf[4, z] + s2_full[z])
    for k in range(OWN):
        value = x_buf[4, k] + s2_full[k] + x_buf[1, k]
        put_natural(stage, value, 2, k)
    outs.append(pltpu.make_async_copy(stage.at[2], relaxed.at[2], out_sem.at[2]))
    outs[2].start()
    phi(first, range(OWN))
    for k in range(OWN):
        value = x_buf[4, k] + s3_own[k] + x_buf[2, k]
        put_natural(stage, value, 3, k)
    outs.append(pltpu.make_async_copy(stage.at[3], relaxed.at[3], out_sem.at[3]))
    outs[3].start()

    r_copy.wait_recv()
    for k in range(OWN):
        put_natural(r_stage, has_before * r_recv[k], k)
    outs.append(pltpu.make_async_copy(r_stage, residual.at[0], out_sem.at[4]))
    outs[4].start()

    for copy in nb_copies:
        copy.wait_recv()
    row = nb[0]
    for i in range(1, levels * COLUMNS):
        row = row + nb[i]
    norm[...] = jnp.broadcast_to(jnp.sum(row, axis=1, keepdims=True), (1, NY))

    for gather in (gather_u, gather_s1, gather_s2, gather_e):
        gather.drain()
    for copy in (a_right_rest, a_left_rest, a_right, a_left, a_on_right, a_on_left, a_give_left, a_give_right, a_give_first, a_give_second):
        copy.wait_send()
    for copy in [part[0] for part in parts] + v_copies + [r_copy, na_copy]:
        copy.wait_send()
    for copy in nb_copies:
        copy.wait_send()
    for copy in outs:
        copy.wait()


def write_out(relaxed, residual, relaxed_out, residual_out, sem):
    copies = [
        pltpu.make_async_copy(relaxed, relaxed_out, sem.at[0]),
        pltpu.make_async_copy(residual, residual_out, sem.at[1]),
    ]
    for copy in copies:
        copy.start()
    for copy in copies:
        copy.wait()


def local(state, source, absorption):
    levels = lax.axis_size("tm") // PLANE
    f32 = jnp.float32
    packed = (NZ, 8, 8, NY)
    any_spec = pl.BlockSpec(memory_space=pl.ANY)
    vm = lambda *shape: pltpu.VMEM(shape, f32)
    dma = lambda *shape: pltpu.SemaphoreType.DMA(shape)
    relaxed, residual, norm = pl.pallas_call(
        kernel,
        out_shape=(
            jax.ShapeDtypeStruct((CF, OWN, NX, NY), f32),
            jax.ShapeDtypeStruct((1, OWN, NX, NY), f32),
            jax.ShapeDtypeStruct((1, NY), f32),
        ),
        in_specs=[any_spec] * 3,
        out_specs=(any_spec, any_spec, pl.BlockSpec(memory_space=pltpu.VMEM)),
        scratch_shapes=[
            vm(*packed), vm(*packed), vm(*packed), vm(*packed),
            vm(OWN, 8, 8, NY), vm(OWN, 8, 8, NY),
            vm(*packed), vm(*packed), vm(*packed), vm(*packed),
            vm(*packed), vm(*packed), vm(*packed), vm(*packed), vm(*packed),
            vm(*packed), vm(*packed), vm(5, *packed),
            vm(6, OWN, NX, NY), vm(2, 8, 8, NY), vm(2, 8, 8, NY),
            vm(OWN, 8, 8, NY), vm(OWN, 8, 8, NY), vm(OWN, 8, 8, NY),
            vm(CF, OWN, NX, NY), vm(OWN, 8, 8, NY), vm(OWN, NX, NY),
            vm(2, 1, NY), vm(levels * COLUMNS, 1, NY),
            dma(6), dma(5), dma(10), dma(10), dma(4, 10), dma(4, 10), dma(4), dma(4), dma(7), dma(7),
            dma(1), dma(1), dma(1), dma(1), dma(levels * COLUMNS - 1), dma(levels * COLUMNS - 1),
            pltpu.SemaphoreType.REGULAR((len(REACHES),)),
        ],
        compiler_params=pltpu.CompilerParams(
            collective_id=0, has_side_effects=True, vmem_limit_bytes=VMEM_BYTES
        ),
    )(*(pltpu.with_memory_space_constraint(array, pltpu.HBM) for array in (state, source, absorption)))
    relaxed, residual = pl.pallas_call(
        write_out,
        out_shape=(jax.ShapeDtypeStruct(relaxed.shape, f32), jax.ShapeDtypeStruct(residual.shape, f32)),
        in_specs=[any_spec] * 2,
        out_specs=(any_spec, any_spec),
        scratch_shapes=[dma(2)],
        compiler_params=pltpu.CompilerParams(vmem_limit_bytes=1024 * 1024),
    )(relaxed, residual)
    return relaxed, residual, norm[0, 0]


def solution(mesh):
    return jax.shard_map(
        local,
        mesh=mesh,
        in_specs=(P("tm", "space", None, None), P("tm", "space", None, None), P("space", None, None)),
        out_specs=(P("tm", "space", None, None), P("tm", "space", None, None), P()),
        check_vma=False,
    )
```

```python
import math

import jax
import jax.numpy as jnp
import numpy as np
from jax import lax
from jax.experimental import pallas as pl
from jax.experimental.pallas import tpu as pltpu
from jax.sharding import PartitionSpec as P

MESH = pl.DeviceIdType.MESH
CF = 4
SWEEPS = 5
COUPLING = 4.0
NZ, NX, NY = 16, 64, 128
OWN = 4
SPACES = 4
PLANE = 8
REACHES = (1, 2, 4, 1)
COLUMNS = 4
HALF = 64
ALL = frozenset(range(16))
VMEM_BYTES = 48 * 1024 * 1024


def sweep_weights(count):
    spread = 6.0 * COUPLING / (1.0 + 6.0 * COUPLING)
    return [
        1.0 / (1.0 + spread * math.cos(math.pi * (2 * k + 1) / (2 * count))) for k in range(count)
    ]


def coefficients():
    poly = np.zeros(SWEEPS + 1)
    poly[0] = 1.0
    for w in sweep_weights(SWEEPS):
        shifted = np.concatenate([[0.0], poly[:-1]])
        poly = (1.0 - w) * poly + w * shifted
        poly[0] += w
    return [float(c) for c in poly]


COEF = coefficients()
C2 = 0.5 * (COEF[2] + COEF[3])
C4 = 0.5 * (COEF[4] + COEF[5])


def grow(layers):
    return frozenset((z + step) % NZ for z in layers for step in (-1, 0, 1))


def kernel(
    state, source, absorption, relaxed, residual, norm,
    a_full, u_full, s1_full, s2_full, s0_own, s3_own,
    rd, q1, q2, q3, d_buf, l1, l2, l3, l4, v_buf, e_full, x_buf,
    loaded, point_buf, rs_left, rs_right, rv_own, rv_left, rv_right, stage, r_recv, r_stage,
    na, nb,
    local_sem, out_sem, a_send, a_recv, ag_send, ag_recv, rs_send, rs_recv, v_send, v_recv,
    r_send, r_recv_sem, na_send, na_recv, nb_send, nb_recv, ready_sem,
):
    c = lax.axis_index("tm")
    d = lax.axis_index("space")
    tms = lax.axis_size("tm")
    levels = tms // PLANE
    after, before = lax.rem(c + 1, tms), lax.rem(c + tms - 1, tms)
    right, left = lax.rem(d + 1, SPACES), lax.rem(d + SPACES - 1, SPACES)
    plane, seat = c // PLANE, lax.rem(c, PLANE)
    core = lax.rem(c, 2)
    partner = c + 1 - 2 * core

    def at(t, s):
        return {"tm": t, "space": s}

    def seat_at(i):
        return plane * PLANE + lax.rem(seat + i, PLANE)

    def level_at(i):
        return lax.rem(plane + i, levels) * PLANE + seat

    def remote(src, dst, send, recv, target):
        return pltpu.make_async_remote_copy(
            src_ref=src, dst_ref=dst, send_sem=send, recv_sem=recv,
            device_id=target, device_id_type=MESH,
        )

    loads = []
    for i, (src, dst) in enumerate([
        (absorption, loaded.at[0]),
        (state.at[0], loaded.at[1]),
        (source.at[1], loaded.at[2]),
        (source.at[2], loaded.at[3]),
        (source.at[0], loaded.at[4]),
        (source.at[3], loaded.at[5]),
    ]):
        copy = pltpu.make_async_copy(src, dst, local_sem.at[i])
        copy.start()
        loads.append(copy)

    barrier = pltpu.get_barrier_semaphore()
    peers = [at(c, left), at(c, right)]
    peers += [at(t, s) for t in (after, before) for s in (d, left, right)]
    peers += [at(seat_at(i), d) for i in range(1, PLANE)]
    peers += [at(level_at(i), d) for i in (1, levels - 1)]
    for peer in peers:
        pl.semaphore_signal(barrier, inc=1, device_id=peer, device_id_type=MESH)

    rows = lax.broadcasted_iota(jnp.int32, (8, NY), 0)
    lane = lax.broadcasted_iota(jnp.int32, (8, NY), 1)
    lanes = lax.broadcasted_iota(jnp.int32, (4, 8, NY), 2) % HALF
    even, lower = lane % 2 == 0, lane < HALF
    split = 2 * (lane % HALF) + lane // HALF
    merge = HALF * (lane % 2) + lane // 2
    inner_up, inner_down = rows != 7, rows != 0
    edge_up, edge_down = (rows == 7) & (lane >= HALF), (rows == 0) & lower

    def pick(x, index):
        return jnp.take_along_axis(x, index, axis=1)
    joined = [jnp.where(d == SPACES - 1 - b, 0.0, 1.0).astype(jnp.float32) for b in range(SPACES)]

    def natural(ref, *index):
        tiles = [[], []]
        for w in range(4):
            top = ref[(*index, pl.ds(w, 8, stride=4), slice(None))]
            low = ref[(*index, pl.ds(NX // 2 + w, 8, stride=4), slice(None))]
            tiles[0].append(pick(jnp.where(even, top, pltpu.roll(low, 1, 1)), split))
            tiles[1].append(pick(jnp.where(even, pltpu.roll(top, NY - 1, 1), low), split))
        return jnp.stack(tiles[0] + tiles[1])

    def put_natural(ref, value, *index):
        for w in range(4):
            first, second = pick(value[w], merge), pick(value[4 + w], merge)
            ref[(*index, pl.ds(w, 8, stride=4), slice(None))] = jnp.where(even, first, pltpu.roll(second, 1, 1))
            ref[(*index, pl.ds(NX // 2 + w, 8, stride=4), slice(None))] = jnp.where(even, pltpu.roll(first, NY - 1, 1), second)

    def ready_signal(number):
        reach = REACHES[number]
        for i in (reach, levels - reach):
            pl.semaphore_signal(ready_sem.at[number], inc=1, device_id=at(level_at(i), d), device_id_type=MESH)

    def ready_wait(number):
        pl.semaphore_wait(ready_sem.at[number], 2)

    class Gather:
        def __init__(self, full, slot):
            self.full, self.slot = full, slot

        def copy(self, src, dst, count, part, target):
            return remote(self.full.at[pl.ds(src, count)], self.full.at[pl.ds(dst, count)],
                          ag_send.at[self.slot, part], ag_recv.at[self.slot, part], at(c, target))

        def prepare(self):
            self.first = [self.copy(0, 12, 1, 0, right), self.copy(2, 6, 1, 1, left),
                          self.copy(1, 13, 1, 2, right), self.copy(3, 7, 1, 3, left)]
            self.rest = [self.copy(2, 14, 2, 4, right), self.copy(0, 4, 2, 5, left)]
            self.onward = [self.copy(12, 8, 1, 6, right), self.copy(6, 10, 1, 7, left),
                           self.copy(13, 9, 1, 8, right), self.copy(7, 11, 1, 9, left)]

        def start(self):
            self.prepare()
            for copy in self.first + self.rest:
                copy.start()

        def forward(self):
            for came, goes in zip(self.first, self.onward):
                came.wait_recv()
                goes.start()

        def middle(self):
            for copy in self.rest:
                copy.wait_recv()

        def finish(self):
            for copy in self.onward:
                copy.wait_recv()

        def drain(self):
            for copy in self.first + self.rest + self.onward:
                copy.wait_send()

    gather_u, gather_s1, gather_s2 = Gather(u_full, 0), Gather(s1_full, 1), Gather(s2_full, 2)
    gather_e = Gather(e_full, 3)

    gather_a = Gather(a_full, 4)

    def a_give(first, count, part):
        return remote(a_full.at[pl.ds(first, count)], a_full.at[pl.ds(first, count)],
                      a_send.at[part], a_recv.at[part], at(partner, d))

    a_gives = [a_give(4, 4, 0), a_give(12, 4, 1), a_give(8, 4, 2)]

    def neighbours(ref, z, have):
        terms = []
        if z in have:
            x = ref[z]
            after_x, before_x = [], []
            for p in range(2):
                up, down = pltpu.roll(x[4 * p], 7, 0), pltpu.roll(x[4 * p + 3], 1, 0)
                across = pltpu.roll(jnp.where(edge_up, up, jnp.where(edge_down, down, 0.0)), HALF, 1)
                up = jnp.where(inner_up, up, across)
                down = jnp.where(inner_down, down, across)
                after_x += [x[4 * p + 1:4 * p + 4], up[None]]
                before_x += [down[None], x[4 * p:4 * p + 3]]
            terms.append(jnp.concatenate(after_x) + jnp.concatenate(before_x))
            evens, odds = x[:4], x[4:]
            terms.append(jnp.concatenate([odds, evens]))
            terms.append(jnp.concatenate([
                jnp.where(lanes == 0, 0.0, pltpu.roll(odds, 1, 2)),
                jnp.where(lanes == HALF - 1, 0.0, pltpu.roll(evens, NY - 1, 2)),
            ]))
        above, below = (z + 1) % NZ, (z - 1) % NZ
        if above in have:
            terms.append(ref[above] if above % OWN else joined[z // OWN] * ref[above])
        if below in have:
            terms.append(ref[below] if z % OWN else joined[below // OWN] * ref[below])
        total = terms[0]
        for term in terms[1:]:
            total = total + term
        return total

    steps = [(d_buf, l1, q1), (l1, l2, q2), (l2, l3, q1), (l3, l4, q3)]

    turn = [0]

    def in_turn(layers):
        turn[0] += 1
        return sorted(layers, key=lambda z: (z - turn[0]) % NZ)

    def level(number, layers, have, have_d):
        src, dst, factor = steps[number - 1]
        for z in in_turn(layers):
            value = factor[z] * neighbours(src, z, have)
            if number % 2 == 0 and z in have_d:
                value = d_buf[z] + value
            dst[z] = value

    def last_step(layers, have, emit, order=None):
        for z in order or in_turn(layers):
            value = q1[z] * neighbours(l4, z, have)
            emit(z, l4[z] + value if z in have else value)

    def phi(emit, want=ALL, order=None):
        need = [frozenset(want)]
        for _ in range(SWEEPS - 1):
            need.insert(0, grow(need[0]))
        for number in range(1, SWEEPS):
            level(number, need[number - 1], ALL, ALL)
        last_step(want, ALL, emit, order)

    def invert(layers):
        for z in layers:
            inverse = 1.0 / (1.0 + 6.0 * COUPLING + a_full[z])
            rd[z] = inverse
            q1[z] = COUPLING * inverse
            q2[z] = (COUPLING * C4 / C2) * inverse
            q3[z] = (COUPLING * C2) * inverse

    def place(full, number):
        loads[number].wait()
        for k in range(OWN):
            full[k] = natural(loaded, number, k)

    place(a_full, 0)
    pl.semaphore_wait(barrier, len(peers))

    gather_a.prepare()

    @pl.when(core == 1)
    def _():
        for copy in gather_a.first + gather_a.rest:
            copy.start()

    ready_signal(0)
    invert(range(4))
    for full, number in ((u_full, 1), (s1_full, 2), (s2_full, 3), (s0_own, 4), (s3_own, 5)):
        place(full, number)
    for k in range(OWN):
        d_buf[k] = rd[k] * u_full[k]

    @pl.when(core == 1)
    def _():
        gather_a.forward()
        gather_a.middle()
        a_gives[0].start()
        a_gives[1].start()

    @pl.when(core == 0)
    def _():
        a_gives[0].wait_recv()
        a_gives[1].wait_recv()

    gather_u.start()
    invert((4, 5, 6, 7, 12, 13, 14, 15))

    reach = [frozenset(range(OWN))]
    for _ in range(SWEEPS):
        reach.append(grow(reach[-1]))
    for number in range(1, SWEEPS):
        level(number, reach[number], reach[number - 1], reach[0])

    def scaled(z, x):
        d_buf[z] = rd[z] * x

    known = ALL - frozenset((8, 9, 10, 11))
    inner = [known]
    for _ in range(1, SWEEPS):
        inner.append(ALL - grow(ALL - inner[-1]))
    last_step(known, reach[SWEEPS - 1], scaled)
    for k in range(OWN):
        d_buf[k] = d_buf[k] + rd[k] * s1_full[k]
    for number in range(1, SWEEPS):
        level(number, inner[number], ALL, ALL)

    @pl.when(core == 1)
    def _():
        gather_a.finish()
        a_gives[2].start()

    @pl.when(core == 0)
    def _():
        a_gives[2].wait_recv()

    ready_wait(0)
    ready_signal(1)
    invert((8, 9, 10, 11))
    for z in (9, 10):
        d_buf[z] = jnp.zeros((8, 8, NY), jnp.float32)
    last_step((8, 11), reach[SWEEPS - 1], scaled)
    for number in range(1, SWEEPS):
        level(number, ALL - inner[number], ALL, ALL)
    last_step(ALL, ALL, scaled)
    for k in range(OWN):
        d_buf[k] = d_buf[k] + rd[k] * s2_full[k]
    gather_u.forward()
    phi(scaled)
    for k in range(OWN):
        d_buf[k] = d_buf[k] + rd[k] * s3_own[k]
    ready_wait(1)
    ready_signal(2)

    parts = []
    for k in range(2):
        parts.append((remote(v_buf.at[pl.ds(8 + k, 1)], rs_left.at[pl.ds(k, 1)],
                             rs_send.at[2 * k], rs_recv.at[2 * k], at(c, right)), 4 + k, rs_left, k))
        parts.append((remote(v_buf.at[pl.ds(10 + k, 1)], rs_right.at[pl.ds(k, 1)],
                             rs_send.at[2 * k + 1], rs_recv.at[2 * k + 1], at(c, left)), 14 + k, rs_right, k))

    def respond(z, x):
        v_buf[z] = x
        if z == 11:
            for part in parts:
                part[0].start()

    phi(respond, ALL, (8, 9, 10, 11, 6, 7, 12, 13, 0, 1, 2, 3, 4, 5, 14, 15))
    v_copies = [
        remote(v_buf.at[pl.ds(0, 4)], rv_own, v_send.at[0], v_recv.at[0], at(after, d)),
        remote(v_buf.at[pl.ds(6, 2)], rv_left.at[pl.ds(2, 2)], v_send.at[1], v_recv.at[1], at(after, right)),
        remote(v_buf.at[pl.ds(12, 2)], rv_right.at[pl.ds(0, 2)], v_send.at[2], v_recv.at[2], at(after, left)),
    ]
    for copy in v_copies:
        copy.start()
    for i, (part, layer, came, k) in enumerate(parts):
        part.wait_recv()
        v_buf[layer] = v_buf[layer] + came[k]
        dst, target = (rv_left, right) if came is rs_left else (rv_right, left)
        copy = remote(v_buf.at[pl.ds(layer, 1)], dst.at[pl.ds(layer - (4 if came is rs_left else 12), 1)],
                      v_send.at[3 + i], v_recv.at[3 + i], at(after, target))
        copy.start()
        v_copies.append(copy)

    gather_u.middle()
    gather_u.finish()
    for z in range(NZ):
        d_buf[z] = rd[z] * u_full[z]

    def first(z, x):
        x_buf[4, z] = x

    phi(first)
    ready_wait(2)
    ready_signal(3)

    for copy in v_copies[:3]:
        copy.wait_recv()
    has_before = jnp.where(c > 0, 1.0, 0.0).astype(jnp.float32)
    gather_e.prepare()
    for k in range(2):
        for copy in v_copies[3 + 2 * k:5 + 2 * k]:
            copy.wait_recv()
        for layer in (k, 2 + k):
            point_buf[layer] = has_before * (rv_own[layer] + rv_left[layer] + rv_right[layer]) + s0_own[layer]
            e_full[layer] = point_buf[layer] - u_full[layer]
        for copy in gather_e.first[2 * k:2 * k + 2]:
            copy.start()
    for copy in gather_e.rest:
        copy.start()
    for k in range(OWN):
        put_natural(stage, point_buf[k], 0, k)
    outs = [pltpu.make_async_copy(stage.at[0], relaxed.at[0], out_sem.at[0])]
    outs[0].start()
    gather_e.forward()
    gather_s1.start()
    gather_e.middle()

    for z in known:
        d_buf[z] = rd[z] * e_full[z]
    for number in range(1, SWEEPS):
        level(number, inner[number], ALL, ALL)
    gather_e.finish()
    for z in ALL - known:
        d_buf[z] = rd[z] * e_full[z]
    for number in range(1, SWEEPS):
        level(number, ALL - inner[number], ALL, ALL)

    def chain(j):
        def emit(z, x):
            x_buf[j, z] = x
            d_buf[z] = rd[z] * x
        return emit

    last_step(ALL, ALL, chain(0))
    phi(chain(1))
    gather_s1.forward()
    gather_s2.start()
    phi(chain(2))
    ready_wait(3)

    squares = []

    def last(z, x):
        if z < OWN:
            x_buf[3, z] = x
        squares.append(x * x)

    phi(last)
    total = squares[0]
    for square in squares[1:]:
        total = total + square
    has_after = jnp.where(c < tms - 1, 1.0, 0.0).astype(jnp.float32)
    na[0] = has_after * jnp.sum(jnp.sum(total, axis=0), axis=0, keepdims=True)
    na_copy = remote(na.at[0], na.at[1], na_send.at[0], na_recv.at[0], at(partner, d))
    na_copy.start()
    r_copy = remote(x_buf.at[3, pl.ds(0, 4)], r_recv, r_send.at[0], r_recv_sem.at[0], at(after, d))
    na_copy.wait_recv()
    nb[0] = na[0] + na[1]
    nb_copies = []
    farthest_first = sorted(range(1, levels * COLUMNS), key=lambda i: -min(i // COLUMNS, levels - i // COLUMNS))
    for i in farthest_first:
        target = lax.rem(plane + i // COLUMNS, levels) * PLANE + lax.rem(seat + 2 * (i % COLUMNS), PLANE)
        copy = remote(nb.at[0], nb.at[i], nb_send.at[i - 1], nb_recv.at[i - 1], at(target, d))
        copy.start()
        nb_copies.append(copy)

    gather_s2.forward()
    gather_s1.middle()
    gather_s1.finish()
    for z in range(NZ):
        d_buf[z] = rd[z] * (x_buf[4, z] + s1_full[z])
    for k in range(OWN):
        value = x_buf[4, k] + s1_full[k] + x_buf[0, k]
        put_natural(stage, value, 1, k)
    outs.append(pltpu.make_async_copy(stage.at[1], relaxed.at[1], out_sem.at[1]))
    outs[1].start()
    near = frozenset(range(OWN))
    for _ in range(SWEEPS):
        near = grow(near)
    phi(first, near)
    r_copy.start()
    gather_s2.middle()
    gather_s2.finish()
    for z in near:
        d_buf[z] = rd[z] * (x_buf[4, z] + s2_full[z])
    for k in range(OWN):
        value = x_buf[4, k] + s2_full[k] + x_buf[1, k]
        put_natural(stage, value, 2, k)
    outs.append(pltpu.make_async_copy(stage.at[2], relaxed.at[2], out_sem.at[2]))
    outs[2].start()
    phi(first, range(OWN))
    for k in range(OWN):
        value = x_buf[4, k] + s3_own[k] + x_buf[2, k]
        put_natural(stage, value, 3, k)
    outs.append(pltpu.make_async_copy(stage.at[3], relaxed.at[3], out_sem.at[3]))
    outs[3].start()

    r_copy.wait_recv()
    for k in range(OWN):
        put_natural(r_stage, has_before * r_recv[k], k)
    outs.append(pltpu.make_async_copy(r_stage, residual.at[0], out_sem.at[4]))
    outs[4].start()

    for copy in nb_copies:
        copy.wait_recv()
    row = nb[0]
    for i in range(1, levels * COLUMNS):
        row = row + nb[i]
    norm[...] = jnp.broadcast_to(jnp.sum(row, axis=1, keepdims=True), (1, NY))

    for gather in (gather_u, gather_s1, gather_s2, gather_e):
        gather.drain()

    @pl.when(core == 1)
    def _():
        gather_a.drain()
        for copy in a_gives:
            copy.wait_send()

    for copy in [part[0] for part in parts] + v_copies + [r_copy, na_copy]:
        copy.wait_send()
    for copy in nb_copies:
        copy.wait_send()
    for copy in outs:
        copy.wait()


def write_out(relaxed, residual, relaxed_out, residual_out, sem):
    copies = [
        pltpu.make_async_copy(relaxed, relaxed_out, sem.at[0]),
        pltpu.make_async_copy(residual, residual_out, sem.at[1]),
    ]
    for copy in copies:
        copy.start()
    for copy in copies:
        copy.wait()


def local(state, source, absorption):
    levels = lax.axis_size("tm") // PLANE
    f32 = jnp.float32
    packed = (NZ, 8, 8, NY)
    any_spec = pl.BlockSpec(memory_space=pl.ANY)
    vm = lambda *shape: pltpu.VMEM(shape, f32)
    dma = lambda *shape: pltpu.SemaphoreType.DMA(shape)
    relaxed, residual, norm = pl.pallas_call(
        kernel,
        out_shape=(
            jax.ShapeDtypeStruct((CF, OWN, NX, NY), f32),
            jax.ShapeDtypeStruct((1, OWN, NX, NY), f32),
            jax.ShapeDtypeStruct((1, NY), f32),
        ),
        in_specs=[any_spec] * 3,
        out_specs=(any_spec, any_spec, pl.BlockSpec(memory_space=pltpu.VMEM)),
        scratch_shapes=[
            vm(*packed), vm(*packed), vm(*packed), vm(*packed),
            vm(OWN, 8, 8, NY), vm(OWN, 8, 8, NY),
            vm(*packed), vm(*packed), vm(*packed), vm(*packed),
            vm(*packed), vm(*packed), vm(*packed), vm(*packed), vm(*packed),
            vm(*packed), vm(*packed), vm(5, *packed),
            vm(6, OWN, NX, NY), vm(OWN, 8, 8, NY), vm(2, 8, 8, NY), vm(2, 8, 8, NY),
            vm(OWN, 8, 8, NY), vm(OWN, 8, 8, NY), vm(OWN, 8, 8, NY),
            vm(CF, OWN, NX, NY), vm(OWN, 8, 8, NY), vm(OWN, NX, NY),
            vm(2, 1, NY), vm(levels * COLUMNS, 1, NY),
            dma(6), dma(5), dma(3), dma(3), dma(5, 10), dma(5, 10), dma(4), dma(4), dma(7), dma(7),
            dma(1), dma(1), dma(1), dma(1), dma(levels * COLUMNS - 1), dma(levels * COLUMNS - 1),
            pltpu.SemaphoreType.REGULAR((len(REACHES),)),
        ],
        compiler_params=pltpu.CompilerParams(
            collective_id=0, has_side_effects=True, vmem_limit_bytes=VMEM_BYTES
        ),
    )(*(pltpu.with_memory_space_constraint(array, pltpu.HBM) for array in (state, source, absorption)))
    relaxed, residual = pl.pallas_call(
        write_out,
        out_shape=(jax.ShapeDtypeStruct(relaxed.shape, f32), jax.ShapeDtypeStruct(residual.shape, f32)),
        in_specs=[any_spec] * 2,
        out_specs=(any_spec, any_spec),
        scratch_shapes=[dma(2)],
        compiler_params=pltpu.CompilerParams(vmem_limit_bytes=1024 * 1024),
    )(relaxed, residual)
    return relaxed, residual, norm[0, 0]


def solution(mesh):
    return jax.shard_map(
        local,
        mesh=mesh,
        in_specs=(P("tm", "space", None, None), P("tm", "space", None, None), P("space", None, None)),
        out_specs=(P("tm", "space", None, None), P("tm", "space", None, None), P()),
        check_vma=False,
    )
```

```python
import math

import jax
import jax.numpy as jnp
import numpy as np
from jax import lax
from jax.experimental import pallas as pl
from jax.experimental.pallas import tpu as pltpu
from jax.sharding import PartitionSpec as P

MESH = pl.DeviceIdType.MESH
CF = 4
SWEEPS = 5
COUPLING = 4.0
NZ, NX, NY = 16, 64, 128
OWN = 4
SPACES = 4
PLANE = 8
REACHES = (1, 2, 4, 1)
COLUMNS = 4
HALF = 64
ALL = frozenset(range(16))
VMEM_BYTES = 48 * 1024 * 1024


def sweep_weights(count):
    spread = 6.0 * COUPLING / (1.0 + 6.0 * COUPLING)
    return [
        1.0 / (1.0 + spread * math.cos(math.pi * (2 * k + 1) / (2 * count))) for k in range(count)
    ]


def coefficients():
    poly = np.zeros(SWEEPS + 1)
    poly[0] = 1.0
    for w in sweep_weights(SWEEPS):
        shifted = np.concatenate([[0.0], poly[:-1]])
        poly = (1.0 - w) * poly + w * shifted
        poly[0] += w
    return [float(c) for c in poly]


COEF = coefficients()
C2 = 0.5 * (COEF[2] + COEF[3])
C4 = 0.5 * (COEF[4] + COEF[5])


def grow(layers):
    return frozenset((z + step) % NZ for z in layers for step in (-1, 0, 1))


def kernel(
    state, source, absorption, relaxed, residual, norm,
    a_full, u_full, s1_full, s2_full, s0_own, s3_own,
    rd, q1, q2, q3, d_buf, l1, l2, l3, l4, v_buf, e_full, x_buf,
    loaded, point_buf, rs_left, rs_right, rv_own, rv_left, rv_right, stage, r_recv, r_stage,
    na, nb,
    local_sem, out_sem, a_send, a_recv, ag_send, ag_recv, rs_send, rs_recv, v_send, v_recv,
    r_send, r_recv_sem, na_send, na_recv, nb_send, nb_recv, ready_sem,
):
    c = lax.axis_index("tm")
    d = lax.axis_index("space")
    tms = lax.axis_size("tm")
    levels = tms // PLANE
    after, before = lax.rem(c + 1, tms), lax.rem(c + tms - 1, tms)
    right, left = lax.rem(d + 1, SPACES), lax.rem(d + SPACES - 1, SPACES)
    plane, seat = c // PLANE, lax.rem(c, PLANE)
    core = lax.rem(c, 2)
    partner = c + 1 - 2 * core

    def at(t, s):
        return {"tm": t, "space": s}

    def seat_at(i):
        return plane * PLANE + lax.rem(seat + i, PLANE)

    def level_at(i):
        return lax.rem(plane + i, levels) * PLANE + seat

    def remote(src, dst, send, recv, target):
        return pltpu.make_async_remote_copy(
            src_ref=src, dst_ref=dst, send_sem=send, recv_sem=recv,
            device_id=target, device_id_type=MESH,
        )

    loads = []
    for i, (src, dst) in enumerate([
        (absorption, loaded.at[0]),
        (state.at[0], loaded.at[1]),
        (source.at[1], loaded.at[2]),
        (source.at[2], loaded.at[3]),
        (source.at[0], loaded.at[4]),
        (source.at[3], loaded.at[5]),
    ]):
        copy = pltpu.make_async_copy(src, dst, local_sem.at[i])
        copy.start()
        loads.append(copy)

    barrier = pltpu.get_barrier_semaphore()
    peers = [at(c, left), at(c, right)]
    peers += [at(t, s) for t in (after, before) for s in (d, left, right)]
    peers += [at(seat_at(i), d) for i in range(1, PLANE)]
    peers += [at(level_at(i), d) for i in (1, levels - 1)]
    for peer in peers:
        pl.semaphore_signal(barrier, inc=1, device_id=peer, device_id_type=MESH)

    rows = lax.broadcasted_iota(jnp.int32, (8, NY), 0)
    lane = lax.broadcasted_iota(jnp.int32, (8, NY), 1)
    lanes = lax.broadcasted_iota(jnp.int32, (4, 8, NY), 2) % HALF
    even, lower = lane % 2 == 0, lane < HALF
    split = 2 * (lane % HALF) + lane // HALF
    merge = HALF * (lane % 2) + lane // 2
    inner_up, inner_down = rows != 7, rows != 0
    edge_up, edge_down = (rows == 7) & (lane >= HALF), (rows == 0) & lower

    def pick(x, index):
        return jnp.take_along_axis(x, index, axis=1)
    joined = [jnp.where(d == SPACES - 1 - b, 0.0, 1.0).astype(jnp.float32) for b in range(SPACES)]

    def natural(ref, *index):
        tiles = [[], []]
        for w in range(4):
            top = ref[(*index, pl.ds(w, 8, stride=4), slice(None))]
            low = ref[(*index, pl.ds(NX // 2 + w, 8, stride=4), slice(None))]
            tiles[0].append(pick(jnp.where(even, top, pltpu.roll(low, 1, 1)), split))
            tiles[1].append(pick(jnp.where(even, pltpu.roll(top, NY - 1, 1), low), split))
        return jnp.stack(tiles[0] + tiles[1])

    def put_natural(ref, value, *index):
        for w in range(4):
            first, second = pick(value[w], merge), pick(value[4 + w], merge)
            ref[(*index, pl.ds(w, 8, stride=4), slice(None))] = jnp.where(even, first, pltpu.roll(second, 1, 1))
            ref[(*index, pl.ds(NX // 2 + w, 8, stride=4), slice(None))] = jnp.where(even, pltpu.roll(first, NY - 1, 1), second)

    def ready_signal(number):
        reach = REACHES[number]
        for i in (reach, levels - reach):
            pl.semaphore_signal(ready_sem.at[number], inc=1, device_id=at(level_at(i), d), device_id_type=MESH)

    def ready_wait(number):
        pl.semaphore_wait(ready_sem.at[number], 2)

    class Gather:
        def __init__(self, full, slot):
            self.full, self.slot = full, slot

        def copy(self, src, dst, count, part, target):
            return remote(self.full.at[pl.ds(src, count)], self.full.at[pl.ds(dst, count)],
                          ag_send.at[self.slot, part], ag_recv.at[self.slot, part], at(c, target))

        def prepare(self):
            self.first = [self.copy(0, 12, 1, 0, right), self.copy(2, 6, 1, 1, left),
                          self.copy(1, 13, 1, 2, right), self.copy(3, 7, 1, 3, left)]
            self.rest = [self.copy(2, 14, 2, 4, right), self.copy(0, 4, 2, 5, left)]
            self.onward = [self.copy(12, 8, 1, 6, right), self.copy(6, 10, 1, 7, left),
                           self.copy(13, 9, 1, 8, right), self.copy(7, 11, 1, 9, left)]

        def start(self):
            self.prepare()
            for copy in self.first + self.rest:
                copy.start()

        def forward(self):
            for came, goes in zip(self.first, self.onward):
                came.wait_recv()
                goes.start()

        def middle(self):
            for copy in self.rest:
                copy.wait_recv()

        def finish(self):
            for copy in self.onward:
                copy.wait_recv()

        def drain(self):
            for copy in self.first + self.rest + self.onward:
                copy.wait_send()

    gather_u, gather_s1, gather_s2 = Gather(u_full, 0), Gather(s1_full, 1), Gather(s2_full, 2)
    gather_e = Gather(e_full, 3)

    gather_a = Gather(a_full, 4)

    def a_give(first, count, part):
        return remote(a_full.at[pl.ds(first, count)], a_full.at[pl.ds(first, count)],
                      a_send.at[part], a_recv.at[part], at(partner, d))

    a_gives = [a_give(4, 4, 0), a_give(12, 4, 1), a_give(8, 4, 2)]

    def neighbours(ref, z, have):
        terms = []
        if z in have:
            x = ref[z]
            after_x, before_x = [], []
            for p in range(2):
                up, down = pltpu.roll(x[4 * p], 7, 0), pltpu.roll(x[4 * p + 3], 1, 0)
                across = pltpu.roll(jnp.where(edge_up, up, jnp.where(edge_down, down, 0.0)), HALF, 1)
                up = jnp.where(inner_up, up, across)
                down = jnp.where(inner_down, down, across)
                after_x += [x[4 * p + 1:4 * p + 4], up[None]]
                before_x += [down[None], x[4 * p:4 * p + 3]]
            terms.append(jnp.concatenate(after_x) + jnp.concatenate(before_x))
            evens, odds = x[:4], x[4:]
            terms.append(jnp.concatenate([odds, evens]))
            terms.append(jnp.concatenate([
                jnp.where(lanes == 0, 0.0, pltpu.roll(odds, 1, 2)),
                jnp.where(lanes == HALF - 1, 0.0, pltpu.roll(evens, NY - 1, 2)),
            ]))
        above, below = (z + 1) % NZ, (z - 1) % NZ
        if above in have:
            terms.append(ref[above] if above % OWN else joined[z // OWN] * ref[above])
        if below in have:
            terms.append(ref[below] if z % OWN else joined[below // OWN] * ref[below])
        total = terms[0]
        for term in terms[1:]:
            total = total + term
        return total

    steps = [(d_buf, l1, q1), (l1, l2, q2), (l2, l3, q1), (l3, l4, q3)]

    turn = [0]

    def in_turn(layers):
        turn[0] += 1
        return sorted(layers, key=lambda z: (z - turn[0]) % NZ)

    def level(number, layers, have, have_d):
        src, dst, factor = steps[number - 1]
        for z in in_turn(layers):
            value = factor[z] * neighbours(src, z, have)
            if number % 2 == 0 and z in have_d:
                value = d_buf[z] + value
            dst[z] = value

    def last_step(layers, have, emit, order=None):
        for z in order or in_turn(layers):
            value = q1[z] * neighbours(l4, z, have)
            emit(z, l4[z] + value if z in have else value)

    def phi(emit, want=ALL, order=None):
        need = [frozenset(want)]
        for _ in range(SWEEPS - 1):
            need.insert(0, grow(need[0]))
        for number in range(1, SWEEPS):
            level(number, need[number - 1], ALL, ALL)
        last_step(want, ALL, emit, order)

    def invert(layers):
        for z in layers:
            inverse = 1.0 / (1.0 + 6.0 * COUPLING + a_full[z])
            rd[z] = inverse
            q1[z] = COUPLING * inverse
            q2[z] = (COUPLING * C4 / C2) * inverse
            q3[z] = (COUPLING * C2) * inverse

    def place(full, number):
        loads[number].wait()
        for k in range(OWN):
            full[k] = natural(loaded, number, k)

    place(a_full, 0)
    pl.semaphore_wait(barrier, len(peers))

    gather_a.prepare()

    @pl.when(core == 1)
    def _():
        for copy in gather_a.first + gather_a.rest:
            copy.start()

    ready_signal(0)
    invert(range(4))
    for full, number in ((u_full, 1), (s1_full, 2), (s2_full, 3), (s0_own, 4), (s3_own, 5)):
        place(full, number)
    for k in range(OWN):
        d_buf[k] = rd[k] * u_full[k]

    @pl.when(core == 1)
    def _():
        gather_a.forward()
        gather_a.middle()
        a_gives[0].start()
        a_gives[1].start()

    @pl.when(core == 0)
    def _():
        a_gives[0].wait_recv()
        a_gives[1].wait_recv()

    gather_u.start()
    invert((4, 5, 6, 7, 12, 13, 14, 15))

    reach = [frozenset(range(OWN))]
    for _ in range(SWEEPS):
        reach.append(grow(reach[-1]))
    for number in range(1, SWEEPS):
        level(number, reach[number], reach[number - 1], reach[0])

    def scaled(z, x):
        d_buf[z] = rd[z] * x

    known = ALL - frozenset((8, 9, 10, 11))
    inner = [known]
    for _ in range(1, SWEEPS):
        inner.append(ALL - grow(ALL - inner[-1]))
    last_step(known, reach[SWEEPS - 1], scaled)
    for k in range(OWN):
        d_buf[k] = d_buf[k] + rd[k] * s1_full[k]
    for number in range(1, SWEEPS):
        level(number, inner[number], ALL, ALL)

    @pl.when(core == 1)
    def _():
        gather_a.finish()
        a_gives[2].start()

    @pl.when(core == 0)
    def _():
        a_gives[2].wait_recv()

    ready_wait(0)
    ready_signal(1)
    invert((8, 9, 10, 11))
    for z in (9, 10):
        d_buf[z] = jnp.zeros((8, 8, NY), jnp.float32)
    last_step((8, 11), reach[SWEEPS - 1], scaled)
    for number in range(1, SWEEPS):
        level(number, ALL - inner[number], ALL, ALL)
    last_step(ALL, ALL, scaled)
    for k in range(OWN):
        d_buf[k] = d_buf[k] + rd[k] * s2_full[k]
    phi(scaled)
    for k in range(OWN):
        d_buf[k] = d_buf[k] + rd[k] * s3_own[k]
    ready_wait(1)
    ready_signal(2)

    parts = []
    for k in range(2):
        parts.append((remote(v_buf.at[pl.ds(8 + k, 1)], rs_left.at[pl.ds(k, 1)],
                             rs_send.at[2 * k], rs_recv.at[2 * k], at(c, right)), 4 + k, rs_left, k))
        parts.append((remote(v_buf.at[pl.ds(10 + k, 1)], rs_right.at[pl.ds(k, 1)],
                             rs_send.at[2 * k + 1], rs_recv.at[2 * k + 1], at(c, left)), 14 + k, rs_right, k))

    def respond(z, x):
        v_buf[z] = x
        if z == 11:
            for part in parts:
                part[0].start()

    gather_u.forward()
    phi(respond, ALL, (8, 9, 10, 11, 6, 7, 12, 13, 0, 1, 2, 3, 4, 5, 14, 15))
    v_copies = [
        remote(v_buf.at[pl.ds(0, 4)], rv_own, v_send.at[0], v_recv.at[0], at(after, d)),
        remote(v_buf.at[pl.ds(6, 2)], rv_left.at[pl.ds(2, 2)], v_send.at[1], v_recv.at[1], at(after, right)),
        remote(v_buf.at[pl.ds(12, 2)], rv_right.at[pl.ds(0, 2)], v_send.at[2], v_recv.at[2], at(after, left)),
    ]
    for copy in v_copies:
        copy.start()
    for i, (part, layer, came, k) in enumerate(parts):
        part.wait_recv()
        v_buf[layer] = v_buf[layer] + came[k]
        dst, target = (rv_left, right) if came is rs_left else (rv_right, left)
        copy = remote(v_buf.at[pl.ds(layer, 1)], dst.at[pl.ds(layer - (4 if came is rs_left else 12), 1)],
                      v_send.at[3 + i], v_recv.at[3 + i], at(after, target))
        copy.start()
        v_copies.append(copy)

    for copy in v_copies[:3]:
        copy.wait_recv()
    has_before = jnp.where(c > 0, 1.0, 0.0).astype(jnp.float32)
    gather_e.prepare()
    for k in range(2):
        for copy in v_copies[3 + 2 * k:5 + 2 * k]:
            copy.wait_recv()
        for layer in (k, 2 + k):
            point_buf[layer] = has_before * (rv_own[layer] + rv_left[layer] + rv_right[layer]) + s0_own[layer]
            e_full[layer] = point_buf[layer] - u_full[layer]
        for copy in gather_e.first[2 * k:2 * k + 2]:
            copy.start()
    for copy in gather_e.rest:
        copy.start()
    for k in range(OWN):
        put_natural(stage, point_buf[k], 0, k)
    outs = [pltpu.make_async_copy(stage.at[0], relaxed.at[0], out_sem.at[0])]
    outs[0].start()
    gather_u.middle()
    gather_u.finish()
    for z in range(NZ):
        d_buf[z] = rd[z] * u_full[z]

    def first(z, x):
        x_buf[4, z] = x

    phi(first)
    ready_wait(2)
    ready_signal(3)

    gather_e.forward()
    gather_s1.start()
    gather_e.middle()

    for z in known:
        d_buf[z] = rd[z] * e_full[z]
    for number in range(1, SWEEPS):
        level(number, inner[number], ALL, ALL)
    gather_e.finish()
    for z in ALL - known:
        d_buf[z] = rd[z] * e_full[z]
    for number in range(1, SWEEPS):
        level(number, ALL - inner[number], ALL, ALL)

    def chain(j):
        def emit(z, x):
            x_buf[j, z] = x
            d_buf[z] = rd[z] * x
        return emit

    last_step(ALL, ALL, chain(0))
    phi(chain(1))
    gather_s1.forward()
    gather_s2.start()
    phi(chain(2))
    ready_wait(3)

    squares = []

    def last(z, x):
        if z < OWN:
            x_buf[3, z] = x
        squares.append(x * x)

    phi(last)
    total = squares[0]
    for square in squares[1:]:
        total = total + square
    has_after = jnp.where(c < tms - 1, 1.0, 0.0).astype(jnp.float32)
    na[0] = has_after * jnp.sum(jnp.sum(total, axis=0), axis=0, keepdims=True)
    na_copy = remote(na.at[0], na.at[1], na_send.at[0], na_recv.at[0], at(partner, d))
    na_copy.start()
    r_copy = remote(x_buf.at[3, pl.ds(0, 4)], r_recv, r_send.at[0], r_recv_sem.at[0], at(after, d))
    na_copy.wait_recv()
    nb[0] = na[0] + na[1]
    nb_copies = []
    farthest_first = sorted(range(1, levels * COLUMNS), key=lambda i: -min(i // COLUMNS, levels - i // COLUMNS))
    for i in farthest_first:
        target = lax.rem(plane + i // COLUMNS, levels) * PLANE + lax.rem(seat + 2 * (i % COLUMNS), PLANE)
        copy = remote(nb.at[0], nb.at[i], nb_send.at[i - 1], nb_recv.at[i - 1], at(target, d))
        copy.start()
        nb_copies.append(copy)

    gather_s2.forward()
    gather_s1.middle()
    gather_s1.finish()
    for z in range(NZ):
        d_buf[z] = rd[z] * (x_buf[4, z] + s1_full[z])
    for k in range(OWN):
        value = x_buf[4, k] + s1_full[k] + x_buf[0, k]
        put_natural(stage, value, 1, k)
    outs.append(pltpu.make_async_copy(stage.at[1], relaxed.at[1], out_sem.at[1]))
    outs[1].start()
    near = frozenset(range(OWN))
    for _ in range(SWEEPS):
        near = grow(near)
    phi(first, near)
    r_copy.start()
    gather_s2.middle()
    gather_s2.finish()
    for z in near:
        d_buf[z] = rd[z] * (x_buf[4, z] + s2_full[z])
    for k in range(OWN):
        value = x_buf[4, k] + s2_full[k] + x_buf[1, k]
        put_natural(stage, value, 2, k)
    outs.append(pltpu.make_async_copy(stage.at[2], relaxed.at[2], out_sem.at[2]))
    outs[2].start()
    phi(first, range(OWN))
    for k in range(OWN):
        value = x_buf[4, k] + s3_own[k] + x_buf[2, k]
        put_natural(stage, value, 3, k)
    outs.append(pltpu.make_async_copy(stage.at[3], relaxed.at[3], out_sem.at[3]))
    outs[3].start()

    r_copy.wait_recv()
    for k in range(OWN):
        put_natural(r_stage, has_before * r_recv[k], k)
    outs.append(pltpu.make_async_copy(r_stage, residual.at[0], out_sem.at[4]))
    outs[4].start()

    for copy in nb_copies:
        copy.wait_recv()
    row = nb[0]
    for i in range(1, levels * COLUMNS):
        row = row + nb[i]
    norm[...] = jnp.broadcast_to(jnp.sum(row, axis=1, keepdims=True), (1, NY))

    for gather in (gather_u, gather_s1, gather_s2, gather_e):
        gather.drain()

    @pl.when(core == 1)
    def _():
        gather_a.drain()
        for copy in a_gives:
            copy.wait_send()

    for copy in [part[0] for part in parts] + v_copies + [r_copy, na_copy]:
        copy.wait_send()
    for copy in nb_copies:
        copy.wait_send()
    for copy in outs:
        copy.wait()


def write_out(relaxed, residual, relaxed_out, residual_out, sem):
    copies = [
        pltpu.make_async_copy(relaxed, relaxed_out, sem.at[0]),
        pltpu.make_async_copy(residual, residual_out, sem.at[1]),
    ]
    for copy in copies:
        copy.start()
    for copy in copies:
        copy.wait()


def local(state, source, absorption):
    levels = lax.axis_size("tm") // PLANE
    f32 = jnp.float32
    packed = (NZ, 8, 8, NY)
    any_spec = pl.BlockSpec(memory_space=pl.ANY)
    vm = lambda *shape: pltpu.VMEM(shape, f32)
    dma = lambda *shape: pltpu.SemaphoreType.DMA(shape)
    relaxed, residual, norm = pl.pallas_call(
        kernel,
        out_shape=(
            jax.ShapeDtypeStruct((CF, OWN, NX, NY), f32),
            jax.ShapeDtypeStruct((1, OWN, NX, NY), f32),
            jax.ShapeDtypeStruct((1, NY), f32),
        ),
        in_specs=[any_spec] * 3,
        out_specs=(any_spec, any_spec, pl.BlockSpec(memory_space=pltpu.VMEM)),
        scratch_shapes=[
            vm(*packed), vm(*packed), vm(*packed), vm(*packed),
            vm(OWN, 8, 8, NY), vm(OWN, 8, 8, NY),
            vm(*packed), vm(*packed), vm(*packed), vm(*packed),
            vm(*packed), vm(*packed), vm(*packed), vm(*packed), vm(*packed),
            vm(*packed), vm(*packed), vm(5, *packed),
            vm(6, OWN, NX, NY), vm(OWN, 8, 8, NY), vm(2, 8, 8, NY), vm(2, 8, 8, NY),
            vm(OWN, 8, 8, NY), vm(OWN, 8, 8, NY), vm(OWN, 8, 8, NY),
            vm(CF, OWN, NX, NY), vm(OWN, 8, 8, NY), vm(OWN, NX, NY),
            vm(2, 1, NY), vm(levels * COLUMNS, 1, NY),
            dma(6), dma(5), dma(3), dma(3), dma(5, 10), dma(5, 10), dma(4), dma(4), dma(7), dma(7),
            dma(1), dma(1), dma(1), dma(1), dma(levels * COLUMNS - 1), dma(levels * COLUMNS - 1),
            pltpu.SemaphoreType.REGULAR((len(REACHES),)),
        ],
        compiler_params=pltpu.CompilerParams(
            collective_id=0, has_side_effects=True, vmem_limit_bytes=VMEM_BYTES
        ),
    )(*(pltpu.with_memory_space_constraint(array, pltpu.HBM) for array in (state, source, absorption)))
    relaxed, residual = pl.pallas_call(
        write_out,
        out_shape=(jax.ShapeDtypeStruct(relaxed.shape, f32), jax.ShapeDtypeStruct(residual.shape, f32)),
        in_specs=[any_spec] * 2,
        out_specs=(any_spec, any_spec),
        scratch_shapes=[dma(2)],
        compiler_params=pltpu.CompilerParams(vmem_limit_bytes=1024 * 1024),
    )(relaxed, residual)
    return relaxed, residual, norm[0, 0]


def solution(mesh):
    return jax.shard_map(
        local,
        mesh=mesh,
        in_specs=(P("tm", "space", None, None), P("tm", "space", None, None), P("space", None, None)),
        out_specs=(P("tm", "space", None, None), P("tm", "space", None, None), P()),
        check_vma=False,
    )
```

```python
import math

import jax
import jax.numpy as jnp
import numpy as np
from jax import lax
from jax.experimental import pallas as pl
from jax.experimental.pallas import tpu as pltpu
from jax.sharding import PartitionSpec as P

MESH = pl.DeviceIdType.MESH
CF = 4
SWEEPS = 5
COUPLING = 4.0
NZ, NX, NY = 16, 64, 128
OWN = 4
SPACES = 4
PLANE = 8
REACHES = (1, 2, 4, 1)
COLUMNS = 4
HALF = 64
ALL = frozenset(range(16))
VMEM_BYTES = 48 * 1024 * 1024


def sweep_weights(count):
    spread = 6.0 * COUPLING / (1.0 + 6.0 * COUPLING)
    return [
        1.0 / (1.0 + spread * math.cos(math.pi * (2 * k + 1) / (2 * count))) for k in range(count)
    ]


def coefficients():
    poly = np.zeros(SWEEPS + 1)
    poly[0] = 1.0
    for w in sweep_weights(SWEEPS):
        shifted = np.concatenate([[0.0], poly[:-1]])
        poly = (1.0 - w) * poly + w * shifted
        poly[0] += w
    return [float(c) for c in poly]


COEF = coefficients()
C2 = 0.5 * (COEF[2] + COEF[3])
C4 = 0.5 * (COEF[4] + COEF[5])


def grow(layers):
    return frozenset((z + step) % NZ for z in layers for step in (-1, 0, 1))


def kernel(
    state, source, absorption, relaxed, residual, norm,
    a_full, u_full, s1_full, s2_full, s0_own, s3_own,
    rd, q1, q2, q3, d_buf, l1, l2, l3, l4, v_buf, e_full, x_buf,
    loaded, point_buf, rs_left, rs_right, rv_own, rv_left, rv_right, stage, r_recv, r_stage,
    na, nb,
    local_sem, out_sem, a_send, a_recv, ag_send, ag_recv, rs_send, rs_recv, v_send, v_recv,
    r_send, r_recv_sem, na_send, na_recv, nb_send, nb_recv, ready_sem,
):
    c = lax.axis_index("tm")
    d = lax.axis_index("space")
    tms = lax.axis_size("tm")
    levels = tms // PLANE
    after, before = lax.rem(c + 1, tms), lax.rem(c + tms - 1, tms)
    right, left = lax.rem(d + 1, SPACES), lax.rem(d + SPACES - 1, SPACES)
    plane, seat = c // PLANE, lax.rem(c, PLANE)
    core = lax.rem(c, 2)
    partner = c + 1 - 2 * core

    def at(t, s):
        return {"tm": t, "space": s}

    def seat_at(i):
        return plane * PLANE + lax.rem(seat + i, PLANE)

    def level_at(i):
        return lax.rem(plane + i, levels) * PLANE + seat

    def remote(src, dst, send, recv, target):
        return pltpu.make_async_remote_copy(
            src_ref=src, dst_ref=dst, send_sem=send, recv_sem=recv,
            device_id=target, device_id_type=MESH,
        )

    loads = []
    for i, (src, dst) in enumerate([
        (absorption, loaded.at[0]),
        (state.at[0], loaded.at[1]),
        (source.at[1], loaded.at[2]),
        (source.at[2], loaded.at[3]),
        (source.at[0], loaded.at[4]),
        (source.at[3], loaded.at[5]),
    ]):
        copy = pltpu.make_async_copy(src, dst, local_sem.at[i])
        copy.start()
        loads.append(copy)

    barrier = pltpu.get_barrier_semaphore()
    peers = [at(c, left), at(c, right)]
    peers += [at(t, s) for t in (after, before) for s in (d, left, right)]
    peers += [at(seat_at(i), d) for i in range(1, PLANE)]
    peers += [at(level_at(i), d) for i in (1, levels - 1)]
    for peer in peers:
        pl.semaphore_signal(barrier, inc=1, device_id=peer, device_id_type=MESH)

    rows = lax.broadcasted_iota(jnp.int32, (8, NY), 0)
    lane = lax.broadcasted_iota(jnp.int32, (8, NY), 1)
    lanes = lax.broadcasted_iota(jnp.int32, (4, 8, NY), 2) % HALF
    even, lower = lane % 2 == 0, lane < HALF
    split = 2 * (lane % HALF) + lane // HALF
    merge = HALF * (lane % 2) + lane // 2
    inner_up, inner_down = rows != 7, rows != 0
    edge_up, edge_down = (rows == 7) & (lane >= HALF), (rows == 0) & lower

    def pick(x, index):
        return jnp.take_along_axis(x, index, axis=1)
    joined = [jnp.where(d == SPACES - 1 - b, 0.0, 1.0).astype(jnp.float32) for b in range(SPACES)]

    def natural(ref, *index):
        tiles = [[], []]
        for w in range(4):
            top = ref[(*index, pl.ds(w, 8, stride=4), slice(None))]
            low = ref[(*index, pl.ds(NX // 2 + w, 8, stride=4), slice(None))]
            tiles[0].append(pick(jnp.where(even, top, pltpu.roll(low, 1, 1)), split))
            tiles[1].append(pick(jnp.where(even, pltpu.roll(top, NY - 1, 1), low), split))
        return jnp.stack(tiles[0] + tiles[1])

    def put_natural(ref, value, *index):
        for w in range(4):
            first, second = pick(value[w], merge), pick(value[4 + w], merge)
            ref[(*index, pl.ds(w, 8, stride=4), slice(None))] = jnp.where(even, first, pltpu.roll(second, 1, 1))
            ref[(*index, pl.ds(NX // 2 + w, 8, stride=4), slice(None))] = jnp.where(even, pltpu.roll(first, NY - 1, 1), second)

    def ready_signal(number):
        reach = REACHES[number]
        for i in (reach, levels - reach):
            pl.semaphore_signal(ready_sem.at[number], inc=1, device_id=at(level_at(i), d), device_id_type=MESH)

    def ready_wait(number):
        pl.semaphore_wait(ready_sem.at[number], 2)

    class Gather:
        def __init__(self, full, slot):
            self.full, self.slot = full, slot

        def copy(self, src, dst, count, part, target):
            return remote(self.full.at[pl.ds(src, count)], self.full.at[pl.ds(dst, count)],
                          ag_send.at[self.slot, part], ag_recv.at[self.slot, part], at(c, target))

        def prepare(self):
            self.first = [self.copy(0, 12, 1, 0, right), self.copy(2, 6, 1, 1, left),
                          self.copy(1, 13, 1, 2, right), self.copy(3, 7, 1, 3, left)]
            self.rest = [self.copy(2, 14, 2, 4, right), self.copy(0, 4, 2, 5, left)]
            self.onward = [self.copy(12, 8, 1, 6, right), self.copy(6, 10, 1, 7, left),
                           self.copy(13, 9, 1, 8, right), self.copy(7, 11, 1, 9, left)]

        def start(self):
            self.prepare()
            for copy in self.first + self.rest:
                copy.start()

        def forward(self):
            for came, goes in zip(self.first, self.onward):
                came.wait_recv()
                goes.start()

        def middle(self):
            for copy in self.rest:
                copy.wait_recv()

        def finish(self):
            for copy in self.onward:
                copy.wait_recv()

        def drain(self):
            for copy in self.first + self.rest + self.onward:
                copy.wait_send()

    gather_u, gather_s1, gather_s2 = Gather(u_full, 0), Gather(s1_full, 1), Gather(s2_full, 2)
    gather_e = Gather(e_full, 3)

    gather_a = Gather(a_full, 4)

    def a_give(first, count, part):
        return remote(a_full.at[pl.ds(first, count)], a_full.at[pl.ds(first, count)],
                      a_send.at[part], a_recv.at[part], at(partner, d))

    a_gives = [a_give(4, 4, 0), a_give(12, 4, 1), a_give(8, 4, 2)]

    def neighbours(ref, z, have):
        terms = []
        if z in have:
            x = ref[z]
            after_x, before_x = [], []
            for p in range(2):
                up, down = pltpu.roll(x[4 * p], 7, 0), pltpu.roll(x[4 * p + 3], 1, 0)
                across = pltpu.roll(jnp.where(edge_up, up, jnp.where(edge_down, down, 0.0)), HALF, 1)
                up = jnp.where(inner_up, up, across)
                down = jnp.where(inner_down, down, across)
                after_x += [x[4 * p + 1:4 * p + 4], up[None]]
                before_x += [down[None], x[4 * p:4 * p + 3]]
            terms.append(jnp.concatenate(after_x) + jnp.concatenate(before_x))
            evens, odds = x[:4], x[4:]
            terms.append(jnp.concatenate([odds, evens]))
            terms.append(jnp.concatenate([
                jnp.where(lanes == 0, 0.0, pltpu.roll(odds, 1, 2)),
                jnp.where(lanes == HALF - 1, 0.0, pltpu.roll(evens, NY - 1, 2)),
            ]))
        above, below = (z + 1) % NZ, (z - 1) % NZ
        if above in have:
            terms.append(ref[above] if above % OWN else joined[z // OWN] * ref[above])
        if below in have:
            terms.append(ref[below] if z % OWN else joined[below // OWN] * ref[below])
        total = terms[0]
        for term in terms[1:]:
            total = total + term
        return total

    steps = [(d_buf, l1, q1), (l1, l2, q2), (l2, l3, q1), (l3, l4, q3)]

    turn = [0]

    def in_turn(layers):
        turn[0] += 1
        return sorted(layers, key=lambda z: (z - turn[0]) % NZ)

    def level(number, layers, have, have_d):
        src, dst, factor = steps[number - 1]
        for z in in_turn(layers):
            value = factor[z] * neighbours(src, z, have)
            if number % 2 == 0 and z in have_d:
                value = d_buf[z] + value
            dst[z] = value

    def last_step(layers, have, emit, order=None):
        for z in order or in_turn(layers):
            value = q1[z] * neighbours(l4, z, have)
            emit(z, l4[z] + value if z in have else value)

    def phi(emit, want=ALL, order=None):
        need = [frozenset(want)]
        for _ in range(SWEEPS - 1):
            need.insert(0, grow(need[0]))
        for number in range(1, SWEEPS):
            level(number, need[number - 1], ALL, ALL)
        last_step(want, ALL, emit, order)

    def invert(layers):
        for z in layers:
            inverse = 1.0 / (1.0 + 6.0 * COUPLING + a_full[z])
            rd[z] = inverse
            q1[z] = COUPLING * inverse
            q2[z] = (COUPLING * C4 / C2) * inverse
            q3[z] = (COUPLING * C2) * inverse

    def place(full, number):
        loads[number].wait()
        for k in range(OWN):
            full[k] = natural(loaded, number, k)

    place(a_full, 0)
    pl.semaphore_wait(barrier, len(peers))

    gather_a.prepare()

    @pl.when(core == 1)
    def _():
        for copy in gather_a.first + gather_a.rest:
            copy.start()

    ready_signal(0)
    invert(range(4))
    for full, number in ((u_full, 1), (s1_full, 2), (s2_full, 3), (s0_own, 4), (s3_own, 5)):
        place(full, number)
    for k in range(OWN):
        d_buf[k] = rd[k] * u_full[k]

    @pl.when(core == 1)
    def _():
        gather_a.forward()
        gather_a.middle()
        a_gives[0].start()
        a_gives[1].start()

    @pl.when(core == 0)
    def _():
        a_gives[0].wait_recv()
        a_gives[1].wait_recv()

    gather_u.start()
    invert((4, 5, 6, 7, 12, 13, 14, 15))

    reach = [frozenset(range(OWN))]
    for _ in range(SWEEPS):
        reach.append(grow(reach[-1]))
    for number in range(1, SWEEPS):
        level(number, reach[number], reach[number - 1], reach[0])

    def scaled(z, x):
        d_buf[z] = rd[z] * x

    known = ALL - frozenset((8, 9, 10, 11))
    inner = [known]
    for _ in range(1, SWEEPS):
        inner.append(ALL - grow(ALL - inner[-1]))
    last_step(known, reach[SWEEPS - 1], scaled)
    for k in range(OWN):
        d_buf[k] = d_buf[k] + rd[k] * s1_full[k]
    for number in range(1, SWEEPS):
        level(number, inner[number], ALL, ALL)

    @pl.when(core == 1)
    def _():
        gather_a.finish()
        a_gives[2].start()

    @pl.when(core == 0)
    def _():
        a_gives[2].wait_recv()

    ready_wait(0)
    ready_signal(1)
    invert((8, 9, 10, 11))
    for z in (9, 10):
        d_buf[z] = jnp.zeros((8, 8, NY), jnp.float32)
    last_step((8, 11), reach[SWEEPS - 1], scaled)
    for number in range(1, SWEEPS):
        level(number, ALL - inner[number], ALL, ALL)
    last_step(ALL, ALL, scaled)
    for k in range(OWN):
        d_buf[k] = d_buf[k] + rd[k] * s2_full[k]
    phi(scaled)
    for k in range(OWN):
        d_buf[k] = d_buf[k] + rd[k] * s3_own[k]
    ready_wait(1)
    ready_signal(2)

    parts = []
    for k in range(2):
        parts.append((remote(v_buf.at[pl.ds(8 + k, 1)], rs_left.at[pl.ds(k, 1)],
                             rs_send.at[2 * k], rs_recv.at[2 * k], at(c, right)), 4 + k, rs_left, k))
        parts.append((remote(v_buf.at[pl.ds(10 + k, 1)], rs_right.at[pl.ds(k, 1)],
                             rs_send.at[2 * k + 1], rs_recv.at[2 * k + 1], at(c, left)), 14 + k, rs_right, k))

    def respond(z, x):
        v_buf[z] = x
        if z == 11:
            for part in parts:
                part[0].start()

    gather_u.forward()
    phi(respond, ALL, (8, 9, 10, 11, 6, 7, 12, 13, 0, 1, 2, 3, 4, 5, 14, 15))
    v_copies = [
        remote(v_buf.at[pl.ds(0, 4)], rv_own, v_send.at[0], v_recv.at[0], at(after, d)),
        remote(v_buf.at[pl.ds(6, 2)], rv_left.at[pl.ds(2, 2)], v_send.at[1], v_recv.at[1], at(after, right)),
        remote(v_buf.at[pl.ds(12, 2)], rv_right.at[pl.ds(0, 2)], v_send.at[2], v_recv.at[2], at(after, left)),
    ]
    for copy in v_copies:
        copy.start()
    for i, (part, layer, came, k) in enumerate(parts):
        part.wait_recv()
        v_buf[layer] = v_buf[layer] + came[k]
        dst, target = (rv_left, right) if came is rs_left else (rv_right, left)
        copy = remote(v_buf.at[pl.ds(layer, 1)], dst.at[pl.ds(layer - (4 if came is rs_left else 12), 1)],
                      v_send.at[3 + i], v_recv.at[3 + i], at(after, target))
        copy.start()
        v_copies.append(copy)

    for copy in v_copies[:3]:
        copy.wait_recv()
    has_before = jnp.where(c > 0, 1.0, 0.0).astype(jnp.float32)
    gather_e.prepare()
    for k in range(2):
        for copy in v_copies[3 + 2 * k:5 + 2 * k]:
            copy.wait_recv()
        for layer in (k, 2 + k):
            point_buf[layer] = has_before * (rv_own[layer] + rv_left[layer] + rv_right[layer]) + s0_own[layer]
            e_full[layer] = point_buf[layer] - u_full[layer]
        for copy in gather_e.first[2 * k:2 * k + 2]:
            copy.start()
    for copy in gather_e.rest:
        copy.start()
    for k in range(OWN):
        put_natural(stage, point_buf[k], 0, k)
    outs = [pltpu.make_async_copy(stage.at[0], relaxed.at[0], out_sem.at[0])]
    outs[0].start()
    gather_u.middle()
    gather_u.finish()
    for z in range(NZ):
        d_buf[z] = rd[z] * u_full[z]

    def first(z, x):
        x_buf[4, z] = x

    phi(first)
    ready_wait(2)
    ready_signal(3)

    gather_e.forward()
    gather_e.middle()
    gather_s1.start()

    for z in known:
        d_buf[z] = rd[z] * e_full[z]
    for number in range(1, SWEEPS):
        level(number, inner[number], ALL, ALL)
    gather_e.finish()
    for z in ALL - known:
        d_buf[z] = rd[z] * e_full[z]
    for number in range(1, SWEEPS):
        level(number, ALL - inner[number], ALL, ALL)

    def chain(j):
        def emit(z, x):
            x_buf[j, z] = x
            d_buf[z] = rd[z] * x
        return emit

    last_step(ALL, ALL, chain(0))
    phi(chain(1))
    phi(chain(2))
    gather_s1.forward()
    gather_s2.start()
    ready_wait(3)

    squares = []

    def last(z, x):
        if z < OWN:
            x_buf[3, z] = x
        squares.append(x * x)

    phi(last)
    total = squares[0]
    for square in squares[1:]:
        total = total + square
    has_after = jnp.where(c < tms - 1, 1.0, 0.0).astype(jnp.float32)
    na[0] = has_after * jnp.sum(jnp.sum(total, axis=0), axis=0, keepdims=True)
    na_copy = remote(na.at[0], na.at[1], na_send.at[0], na_recv.at[0], at(partner, d))
    na_copy.start()
    r_copy = remote(x_buf.at[3, pl.ds(0, 4)], r_recv, r_send.at[0], r_recv_sem.at[0], at(after, d))
    na_copy.wait_recv()
    nb[0] = na[0] + na[1]
    nb_copies = []
    farthest_first = sorted(range(1, levels * COLUMNS), key=lambda i: -min(i // COLUMNS, levels - i // COLUMNS))
    for i in farthest_first:
        target = lax.rem(plane + i // COLUMNS, levels) * PLANE + lax.rem(seat + 2 * (i % COLUMNS), PLANE)
        copy = remote(nb.at[0], nb.at[i], nb_send.at[i - 1], nb_recv.at[i - 1], at(target, d))
        copy.start()
        nb_copies.append(copy)

    gather_s2.forward()
    gather_s1.middle()
    gather_s1.finish()
    for z in range(NZ):
        d_buf[z] = rd[z] * (x_buf[4, z] + s1_full[z])
    for k in range(OWN):
        value = x_buf[4, k] + s1_full[k] + x_buf[0, k]
        put_natural(stage, value, 1, k)
    outs.append(pltpu.make_async_copy(stage.at[1], relaxed.at[1], out_sem.at[1]))
    outs[1].start()
    near = frozenset(range(OWN))
    for _ in range(SWEEPS):
        near = grow(near)
    phi(first, near)
    r_copy.start()
    gather_s2.middle()
    gather_s2.finish()
    for z in near:
        d_buf[z] = rd[z] * (x_buf[4, z] + s2_full[z])
    for k in range(OWN):
        value = x_buf[4, k] + s2_full[k] + x_buf[1, k]
        put_natural(stage, value, 2, k)
    outs.append(pltpu.make_async_copy(stage.at[2], relaxed.at[2], out_sem.at[2]))
    outs[2].start()
    phi(first, range(OWN))
    for k in range(OWN):
        value = x_buf[4, k] + s3_own[k] + x_buf[2, k]
        put_natural(stage, value, 3, k)
    outs.append(pltpu.make_async_copy(stage.at[3], relaxed.at[3], out_sem.at[3]))
    outs[3].start()

    r_copy.wait_recv()
    for k in range(OWN):
        put_natural(r_stage, has_before * r_recv[k], k)
    outs.append(pltpu.make_async_copy(r_stage, residual.at[0], out_sem.at[4]))
    outs[4].start()

    for copy in nb_copies:
        copy.wait_recv()
    row = nb[0]
    for i in range(1, levels * COLUMNS):
        row = row + nb[i]
    norm[...] = jnp.broadcast_to(jnp.sum(row, axis=1, keepdims=True), (1, NY))

    for gather in (gather_u, gather_s1, gather_s2, gather_e):
        gather.drain()

    @pl.when(core == 1)
    def _():
        gather_a.drain()
        for copy in a_gives:
            copy.wait_send()

    for copy in [part[0] for part in parts] + v_copies + [r_copy, na_copy]:
        copy.wait_send()
    for copy in nb_copies:
        copy.wait_send()
    for copy in outs:
        copy.wait()


def write_out(relaxed, residual, relaxed_out, residual_out, sem):
    copies = [
        pltpu.make_async_copy(relaxed, relaxed_out, sem.at[0]),
        pltpu.make_async_copy(residual, residual_out, sem.at[1]),
    ]
    for copy in copies:
        copy.start()
    for copy in copies:
        copy.wait()


def local(state, source, absorption):
    levels = lax.axis_size("tm") // PLANE
    f32 = jnp.float32
    packed = (NZ, 8, 8, NY)
    any_spec = pl.BlockSpec(memory_space=pl.ANY)
    vm = lambda *shape: pltpu.VMEM(shape, f32)
    dma = lambda *shape: pltpu.SemaphoreType.DMA(shape)
    relaxed, residual, norm = pl.pallas_call(
        kernel,
        out_shape=(
            jax.ShapeDtypeStruct((CF, OWN, NX, NY), f32),
            jax.ShapeDtypeStruct((1, OWN, NX, NY), f32),
            jax.ShapeDtypeStruct((1, NY), f32),
        ),
        in_specs=[any_spec] * 3,
        out_specs=(any_spec, any_spec, pl.BlockSpec(memory_space=pltpu.VMEM)),
        scratch_shapes=[
            vm(*packed), vm(*packed), vm(*packed), vm(*packed),
            vm(OWN, 8, 8, NY), vm(OWN, 8, 8, NY),
            vm(*packed), vm(*packed), vm(*packed), vm(*packed),
            vm(*packed), vm(*packed), vm(*packed), vm(*packed), vm(*packed),
            vm(*packed), vm(*packed), vm(5, *packed),
            vm(6, OWN, NX, NY), vm(OWN, 8, 8, NY), vm(2, 8, 8, NY), vm(2, 8, 8, NY),
            vm(OWN, 8, 8, NY), vm(OWN, 8, 8, NY), vm(OWN, 8, 8, NY),
            vm(CF, OWN, NX, NY), vm(OWN, 8, 8, NY), vm(OWN, NX, NY),
            vm(2, 1, NY), vm(levels * COLUMNS, 1, NY),
            dma(6), dma(5), dma(3), dma(3), dma(5, 10), dma(5, 10), dma(4), dma(4), dma(7), dma(7),
            dma(1), dma(1), dma(1), dma(1), dma(levels * COLUMNS - 1), dma(levels * COLUMNS - 1),
            pltpu.SemaphoreType.REGULAR((len(REACHES),)),
        ],
        compiler_params=pltpu.CompilerParams(
            collective_id=0, has_side_effects=True, vmem_limit_bytes=VMEM_BYTES
        ),
    )(*(pltpu.with_memory_space_constraint(array, pltpu.HBM) for array in (state, source, absorption)))
    relaxed, residual = pl.pallas_call(
        write_out,
        out_shape=(jax.ShapeDtypeStruct(relaxed.shape, f32), jax.ShapeDtypeStruct(residual.shape, f32)),
        in_specs=[any_spec] * 2,
        out_specs=(any_spec, any_spec),
        scratch_shapes=[dma(2)],
        compiler_params=pltpu.CompilerParams(vmem_limit_bytes=1024 * 1024),
    )(relaxed, residual)
    return relaxed, residual, norm[0, 0]


def solution(mesh):
    return jax.shard_map(
        local,
        mesh=mesh,
        in_specs=(P("tm", "space", None, None), P("tm", "space", None, None), P("space", None, None)),
        out_specs=(P("tm", "space", None, None), P("tm", "space", None, None), P()),
        check_vma=False,
    )
```
